32 devices in a mesh: ctx: 8 (over y, x, core), dp: 4 (over z).
Axes of the slice: x: 2, y: 2, z: 4, core: 2. Of those that a mesh axis runs over, the one named last changes fastest.
Arguments:
- query: bfloat16 [4, 1024, 512], P('dp', 'ctx'), may hold values from -6 to 6
- key_input: bfloat16 [4, 1024, 512], P('dp', 'ctx'), may hold values from -6 to 6
- value_input: bfloat16 [4, 1024, 512], P('dp', 'ctx'), may hold values from -6 to 6
- filter_taps: float32 [1024, 512], P('ctx'), may hold values from -6 to 6
- grad_output: bfloat16 [4, 1024, 512], P('dp', 'ctx'), may hold values from -6 to 6
Outputs:
- output: bfloat16 [4, 1024, 512], P('dp', 'ctx')
- grad_query: bfloat16 [4, 1024, 512], P('dp', 'ctx')
- grad_key: bfloat16 [4, 1024, 512], P('dp', 'ctx')
- grad_value: bfloat16 [4, 1024, 512], P('dp', 'ctx')
- grad_filter: float32 [1024, 512], P('ctx')
The draws below stay inside these ranges and needn't reach their ends.
All inputs are finite; a program needn't handle non-finite values.
Results may differ from the reference program's by a relative error of at most 0.0058.
Values may be sent and summed in bfloat16 or wider, within the bound.
A program may use at most 64 MiB of HBM per device.

```python
import jax
import jax.numpy as jnp
from jax import lax

C = 512
FILTER_LENGTH = 1024
SEQS = 4


def draw_filter_taps(key, part):
    keys = jax.random.split(jax.random.fold_in(key, 71), 4)
    steps = jnp.arange(FILTER_LENGTH, dtype=jnp.float32)
    scales = jnp.exp(jax.random.uniform(keys[0], (C,), jnp.float32, jnp.log(30.0), jnp.log(4.0 * FILTER_LENGTH)))
    noise = jnp.clip(jax.random.normal(keys[1], (FILTER_LENGTH, C), jnp.float32), -6.0, 6.0)
    shard_positions = jax.random.randint(keys[2], (4,), 1, FILTER_LENGTH)
    twiddle_factors = jax.random.uniform(keys[3], (4, C), jnp.float32, 0.5, 0.8)
    log_decay_envelope = -steps[:, None] / scales[None, :]
    for pulse_train in range(4):
        received_block = (jnp.arange(FILTER_LENGTH, dtype=jnp.int32) >= shard_positions[pulse_train]).astype(jnp.float32)
        log_decay_envelope = log_decay_envelope + received_block[:, None] * jnp.log(twiddle_factors[pulse_train])[None, :]
    envelope = jnp.exp(log_decay_envelope)
    norming = 1.0 / jnp.sqrt(jnp.sum(envelope * envelope, axis=0))
    return noise * envelope * norming[None, :]


def levels(stream_key, shape, cuts, least, top_value):
    loudness, own = 1.0, jax.random.fold_in(stream_key, 6)
    for dim, shards_of in cuts:
        draws = jnp.exp(jax.random.uniform(jax.random.fold_in(own, dim), (shards_of,), jnp.float32, least / len(cuts), top_value / len(cuts)))
        loudness = loudness * jnp.repeat(draws, shape[dim] // shards_of).reshape([-1 if axis == dim else 1 for axis in range(len(shape))])
    return loudness


def gaussian(stream_key, shape, deviation, reach, cuts=(), held_as=jnp.bfloat16):
    array = jax.random.normal(stream_key, shape, jnp.float32) * deviation
    if len(cuts) > 0:
        array = levels(stream_key, shape, cuts, -0.22, 0.18) * array
    return jnp.clip(array, min=-reach, max=reach).astype(held_as)


def setup_inputs(seed: int = 0) -> dict:
    key_list = jax.random.split(jax.random.key(seed), 6)
    return {
        "query": gaussian(key_list[0], (SEQS, FILTER_LENGTH, C), 1.0, 6.0, ((0, 4), (1, 8))),
        "key_input": gaussian(key_list[1], (SEQS, FILTER_LENGTH, C), 1.0, 6.0, ((0, 4), (1, 8))),
        "value_input": gaussian(key_list[2], (SEQS, FILTER_LENGTH, C), 1.0, 6.0, ((0, 4), (1, 8))),
        "filter_taps": draw_filter_taps(jax.random.fold_in(key_list[5], 71), 0),
        "grad_output": gaussian(key_list[4], (SEQS, FILTER_LENGTH, C), 1.0, 6.0, ((0, 4), (1, 8))),
    }


def one_sequence(filter_spec, padded, pieces):
    query, key_input, value_input, grad_output = pieces
    length = query.shape[0]
    product = lax.optimization_barrier((key_input.astype(jnp.float32) * value_input.astype(jnp.float32)).astype(jnp.bfloat16))
    grad_mix = lax.optimization_barrier((grad_output.astype(jnp.float32) * query.astype(jnp.float32)).astype(jnp.bfloat16))
    prod_spec = jnp.fft.rfft(product.astype(jnp.float32), n=padded, axis=0)
    mix_spec = jnp.fft.rfft(grad_mix.astype(jnp.float32), n=padded, axis=0)
    mixed = jnp.fft.irfft(filter_spec * prod_spec, n=padded, axis=0)[:length]
    mixed = lax.optimization_barrier(mixed.astype(jnp.bfloat16)).astype(jnp.float32)
    output = (query.astype(jnp.float32) * mixed).astype(jnp.bfloat16)
    grad_query = (grad_output.astype(jnp.float32) * mixed).astype(jnp.bfloat16)
    grad_product = jnp.fft.irfft(mix_spec * jnp.conj(filter_spec), n=padded, axis=0)[:length]
    grad_product = lax.optimization_barrier(grad_product.astype(jnp.bfloat16)).astype(jnp.float32)
    grad_key = (grad_product * value_input.astype(jnp.float32)).astype(jnp.bfloat16)
    grad_value = (grad_product * key_input.astype(jnp.float32)).astype(jnp.bfloat16)
    grad_taps = jnp.fft.irfft(mix_spec * jnp.conj(prod_spec), n=padded, axis=0)[:length].astype(jnp.float32)
    return output, grad_query, grad_key, grad_value, grad_taps


def reference(query, key_input, value_input, filter_taps, grad_output):
    length = query.shape[1]
    padded = 2 * length
    filter_spec = jnp.fft.rfft(filter_taps, n=padded, axis=0)
    results = lax.map(lambda pieces: one_sequence(filter_spec, padded, pieces), (query, key_input, value_input, grad_output))
    output, grad_query, grad_key, grad_value, grad_taps = results
    grad_filter = jnp.sum(grad_taps, axis=0).astype(jnp.float32)
    return output, grad_query, grad_key, grad_value, grad_filter
```

```python
import functools
import math

import jax
import jax.numpy as jnp
import numpy as np
from jax import lax
from jax.experimental import pallas as pl
from jax.experimental.pallas import tpu as pltpu
from jax.sharding import PartitionSpec as P

HIGH = lax.Precision.HIGHEST
MESH = pl.DeviceIdType.MESH
LANES = 128
VMEM_BYTES = 67043328
F32 = jnp.float32
BF16 = jnp.bfloat16


def block_tables(length):
    odd = 2 * np.arange(length, dtype=np.int64)[:, None] + 1
    angle = (odd * np.arange(length, dtype=np.int64)[None, :] % (4 * length)) * (2.0 * math.pi / (4 * length))
    ahead = np.concatenate([np.cos(angle), -np.sin(angle)], axis=0).astype(np.float32)
    back = ahead.T / np.float32(length)

    def split(table):
        high = jnp.asarray(table).astype(BF16)
        low = (jnp.asarray(table) - high.astype(F32)).astype(BF16)
        return high, low

    with jax.ensure_compile_time_eval():
        ahead_high, ahead_low = split(ahead)
        back_high, back_low = split(back)
        return (
            np.asarray(jnp.concatenate([ahead_high, ahead_low], axis=1)),
            np.asarray(jnp.concatenate([back_high, back_low], axis=1)),
        )


def groups(rows, dtype):
    kind = jnp.int16 if dtype == BF16 else jnp.int32
    lane = lax.broadcasted_iota(kind, (rows, LANES), 1)
    low = lane < LANES // 2
    even = (lane < LANES // 4) | ((lane >= LANES // 2) & (lane < 3 * LANES // 4))
    return low, even


def turn(a, b, c, d, masks):
    low, even = masks

    def halves(first, second):
        turned = pltpu.roll(jnp.where(low, second, first), LANES // 2, 1)
        return jnp.where(low, first, turned), jnp.where(low, turned, second)

    def quarters(first, second):
        return (
            jnp.where(even, first, pltpu.roll(second, LANES // 4, 1)),
            jnp.where(even, pltpu.roll(first, LANES - LANES // 4, 1), second),
        )

    (a, c), (b, d) = halves(a, c), halves(b, d)
    return quarters(a, b) + quarters(c, d)


def turn_rows(tile, masks):
    rows = tile.shape[0] // 4
    return turn(*[tile[n * rows : (n + 1) * rows] for n in range(4)], masks)


def flip(index, mask):
    out, bit = index, 1
    while bit <= mask:
        if mask & bit:
            out = out + bit * (1 - 2 * lax.rem(index // bit, 2))
        bit = 2 * bit
    return out


def total(terms):
    out = None
    for term in terms:
        out = term if out is None else out + term
    return out


def kernel(
    nctx,
    ndp,
    q_hbm,
    k_hbm,
    v_hbm,
    f_hbm,
    g_hbm,
    ahead_hbm,
    back_hbm,
    mx_rx,
    mg_rx,
    g2_rx,
    qv,
    kv,
    vv,
    gv,
    fv,
    ahead_v,
    back_v,
    sendx,
    sendg,
    sendf,
    rxx,
    rxg,
    rxf,
    sigx,
    sigg,
    rigx,
    rigg,
    wei,
    othx,
    othg,
    acc,
    gfs,
    g2_send,
    mx_send,
    mg_send,
    known,
    load_sem,
    x_ssem,
    x_rsem,
    g_ssem,
    g_rsem,
    f_ssem,
    f_rsem,
    g2_ssem,
    g2_rsem,
    mx_ssem,
    mx_rsem,
    mg_ssem,
    mg_rsem,
):
    me = lax.axis_index("ctx")
    row = lax.axis_index("dp")
    length = qv.shape[1]
    ql = length // 4
    tiles = nctx // 2
    part = lax.rem(row, 2)
    base = row - part
    other = base + 1 - part
    mine = 2 * me + part
    slot = (row // 2) * 2 * nctx + mine

    pairs = ((k_hbm, kv), (v_hbm, vv), (g_hbm, gv), (q_hbm, qv), (f_hbm, fv), (ahead_hbm, ahead_v), (back_hbm, back_v))
    loads = [pltpu.make_async_copy(src, dst, load_sem.at[n]) for n, (src, dst) in enumerate(pairs)]
    for load in loads:
        load.start()

    def at(ctx, dp):
        return {"ctx": ctx, "dp": dp}

    inner = jnp.logical_and(part == 1, row + 1 < ndp)
    outer = jnp.logical_and(part == 0, row > 0)
    across = row + 2 * part - 1
    border = jnp.logical_or(inner, outer)
    barrier = pltpu.get_barrier_semaphore()
    pals = [(other, me)] + [(r, flip(me, o)) for o in range(1, nctx) for r in (row, other)]
    for r, c in pals:
        pl.semaphore_signal(barrier, inc=1, device_id=at(c, r), device_id_type=MESH)

    @pl.when(border)
    def _():
        pl.semaphore_signal(barrier, inc=1, device_id=at(me, across), device_id_type=MESH)

    masks_q = groups(ql, BF16)

    def prepare(a_ref, b_ref, into):
        for p in range(tiles):
            cols = slice(p * LANES, (p + 1) * LANES)
            tile = (a_ref[0, :, cols].astype(F32) * b_ref[0, :, cols].astype(F32)).astype(BF16)
            for n, piece in enumerate(turn_rows(tile, masks_q)):
                into[4 * p + n] = piece

    for load in loads[:2]:
        load.wait()
    prepare(kv, vv, sendx)
    rxx[mine] = sendx[mine]
    pl.semaphore_wait(barrier, len(pals) + jnp.where(border, 1, 0))

    def remote(src, dst, ssem, rsem, ctx, dp):
        return pltpu.make_async_remote_copy(
            src_ref=src, dst_ref=dst, send_sem=ssem, recv_sem=rsem, device_id=at(ctx, dp), device_id_type=MESH
        )

    def tile_copy(src, dst, ssem, rsem):
        def copy(ctx, dp, into):
            to = 2 * ctx + lax.rem(dp, 2)
            return remote(src.at[to], dst.at[into], ssem, rsem, ctx, dp)

        def whole():
            every = pl.ds(0, len(pals))
            return remote(src.at[every], dst.at[every], ssem, rsem, me, other)

        return copy, whole

    copy_x, all_x = tile_copy(sendx, rxx, x_ssem, x_rsem)
    copy_g, all_g = tile_copy(sendg, rxg, g_ssem, g_rsem)
    copy_mx, all_mx = tile_copy(mx_send, mx_rx, mx_ssem, mx_rsem)
    copy_mg, all_mg = tile_copy(mg_send, mg_rx, mg_ssem, mg_rsem)

    def copy_f(ctx, into):
        return remote(sendf.at[2 * ctx + part], rxf.at[into], f_ssem, f_rsem, ctx, row)

    def copy_g2(ctx, dp, into):
        return remote(g2_send.at[ctx], g2_rx.at[into], g2_ssem, g2_rsem, ctx, dp)

    def all_f():
        every = pl.ds(0, nctx - 1)
        return remote(sendf.at[every], rxf.at[every], f_ssem, f_rsem, me, other)

    def all_g2():
        every = pl.ds(0, nctx * ndp - 1)
        return remote(g2_rx.at[every], g2_rx.at[every], g2_ssem, g2_rsem, me, other)

    for r, c in pals:
        copy_x(c, r, mine).start()

    @pl.when(border)
    def _():
        pl.semaphore_signal(known, inc=1, device_id=at(me, across), device_id_type=MESH)

    others = [k + jnp.where(me <= k, 1, 0) for k in range(nctx - 1)]
    rows_away = [k + jnp.where(row <= k, 1, 0) for k in range(ndp - 1)]

    def spread_grads():
        for load in loads[2:4]:
            load.wait()
        prepare(gv, qv, sendg)
        rxg[mine] = sendg[mine]
        for r, c in pals:
            copy_g(c, r, mine).start()

    def spread_taps():
        loads[4].wait()
        for p in range(tiles):
            for n, piece in enumerate(turn_rows(fv[:, p * LANES : (p + 1) * LANES].astype(BF16), masks_q)):
                sendf[4 * p + n] = piece
        rxf[me] = sendf[mine]
        for o in range(1, nctx):
            copy_f(flip(me, o), me).start()

    def greet():
        for load in loads[5:]:
            load.wait()
        pl.semaphore_wait(known, 1)

        @pl.when(border)
        def _():
            pl.semaphore_signal(known, inc=1, device_id=at(me, other), device_id_type=MESH)

    def transform(z):
        return jnp.dot(ahead_v[...], jnp.concatenate([z, z], axis=0), preferred_element_type=F32)

    def analyse(whole, rx, sig, rig):
        whole().wait_recv()
        for p in range(0, tiles, 2):
            z = [jnp.concatenate(turn(*[rx[4 * q + n] for n in range(4)], masks_q), axis=0) for q in (p, p + 1)]
            spec = transform(jnp.concatenate(z, axis=1))
            for k in range(2):
                half = spec[:, k * LANES : (k + 1) * LANES]
                sig[p + k] = half
                rig[p + k] = pltpu.roll(half, LANES // 2, 1)

    low, _ = groups(8, F32)
    parity = lax.rem(lax.broadcasted_iota(jnp.int32, (8, LANES), 0), 2)
    alt = jnp.where(parity == 0, 1.0, -1.0).astype(F32)
    zero = jnp.zeros((8, LANES), F32)

    def windows(re, im):
        x_re = [zero] + [sigx[p, re, :] for p in range(tiles)]
        x_im = [zero] + [sigx[p, im, :] for p in range(tiles)]
        r_re = [zero] + [rigx[p, re, :] for p in range(tiles)]
        r_im = [zero] + [rigx[p, im, :] for p in range(tiles)]
        z_re, z_im = [[], []], [[], []]
        for p in range(tiles):
            before_re, before_im = jnp.where(low, r_re[p], r_re[p + 1]), jnp.where(low, r_im[p], r_im[p + 1])
            z_re[0].append(x_re[p + 1] - alt * before_im)
            z_im[0].append(x_im[p + 1] + alt * before_re)
            z_re[1].append(before_re - alt * x_im[p] if p else before_re)
            z_im[1].append(before_im + alt * x_re[p] if p else before_im)
        return z_re, z_im

    def rows_at(i, start):
        return pl.ds(pl.multiple_of(start + i * 8, 8), 8)

    def correlate():
        @pl.loop(0, length // 8, unroll=2)
        def _(i):
            re, im = rows_at(i, 0), rows_at(i, length)
            z_re, z_im = windows(re, im)
            g_re = [sigg[p, re, :] for p in range(tiles)]
            g_im = [sigg[p, im, :] for p in range(tiles)]
            for j in range(nctx):
                b_re, b_im = z_re[j % 2], z_im[j % 2]
                ms = [(m, m - j // 2) for m in range(j // 2, tiles)]
                acc[j, re, :] = total(g_re[m] * b_re[k] + g_im[m] * b_im[k] for m, k in ms)
                acc[j, im, :] = total(g_im[m] * b_re[k] - g_re[m] * b_im[k] for m, k in ms)

        low_f, even_f = groups(64, F32)

        def swing(here, there):
            return pltpu.roll(jnp.where(low_f, here, there), LANES // 2, 1)

        for m in range(0, 2 * length, 64):
            rows = slice(m, m + 64)
            for n in range(nctx // 4):
                a, b, c, d = [acc[4 * n + k, rows, :] for k in range(4)]
                a = jnp.where(low_f, a, c) + swing(c, a)
                b = jnp.where(low_f, b, d) + swing(d, b)
                a = a + pltpu.roll(a, LANES - LANES // 4, 1)
                b = b + pltpu.roll(b, LANES // 4, 1)
                gfs[rows, n * LANES : (n + 1) * LANES] = jnp.where(even_f, a, b).astype(BF16)

    def inverse(high):
        return jnp.dot(back_v[...], jnp.concatenate([high, high], axis=0), preferred_element_type=F32).astype(BF16)

    def send_taps(rows):
        taps = inverse(gfs[...])
        for n in range(nctx // 4):
            for m, piece in enumerate(turn_rows(taps[:, n * LANES : (n + 1) * LANES], masks_q)):
                g2_send[4 * n + m] = piece
        g2_rx[slot] = g2_send[me]
        for r in rows_away:
            copy_g2(me, r, slot).start()
        for r in rows:
            for c in others:
                copy_g2(c, r, slot).start()

    def weigh():
        all_f().wait_recv()
        low_q, even_q = masks_q
        for p in range(tiles):
            z = []
            for k in range(2):
                fa = rxf[2 * p + k]
                turned = pltpu.roll(fa, LANES // 2, 1)
                pieces = []
                for half in (jnp.where(low_q, fa, turned), jnp.where(low_q, turned, fa)):
                    pieces.append(jnp.where(even_q, half, pltpu.roll(half, LANES // 4, 1)))
                    pieces.append(jnp.where(even_q, pltpu.roll(half, LANES - LANES // 4, 1), half))
                z.append(jnp.concatenate(pieces, axis=0))
            wei[p] = transform(jnp.concatenate(z, axis=1))

    def weights(re, im):
        return [[wei[j // 2, rows, pl.ds((j % 2) * LANES, LANES)] for j in range(nctx)] for rows in (re, im)]

    def over_rows(oth, halves):
        @pl.loop(0, length // 16)
        def _(i):
            outs = [halves(rows_at(2 * i + k, 0), rows_at(2 * i + k, length)) for k in range(2)]
            for p in range(tiles):
                for n, start in enumerate((0, length)):
                    rows = pl.ds(pl.multiple_of(start + i * 16, 16), 16)
                    oth[p, rows, :] = jnp.concatenate([outs[0][n][p], outs[1][n][p]], axis=0).astype(BF16)

    def mix_x(re, im):
        w_re, w_im = weights(re, im)
        z_re, z_im = windows(re, im)
        o_re, o_im = [], []
        for p in range(tiles):
            js = [(j, j % 2, p - j // 2) for j in range(2 * p + 2)]
            o_re.append(total(w_re[j] * z_re[h][k] - w_im[j] * z_im[h][k] for j, h, k in js))
            o_im.append(total(w_re[j] * z_im[h][k] + w_im[j] * z_re[h][k] for j, h, k in js))
        return o_re, o_im

    def mix_g(re, im):
        w_re, w_im = weights(re, im)
        g_re = [sigg[p, re, :] for p in range(tiles)]
        g_im = [sigg[p, im, :] for p in range(tiles)]
        r_re = [rigg[p, re, :] for p in range(tiles)] + [zero]
        r_im = [rigg[p, im, :] for p in range(tiles)] + [zero]
        z_re, z_im = [[], []], [[], []]
        for p in range(tiles):
            after_re, after_im = jnp.where(low, r_re[p], r_re[p + 1]), jnp.where(low, r_im[p], r_im[p + 1])
            z_re[0].append(g_re[p] + alt * after_im)
            z_im[0].append(g_im[p] - alt * after_re)
            z_re[1].append(after_re + alt * g_im[p + 1] if p + 1 < tiles else after_re)
            z_im[1].append(after_im - alt * g_re[p + 1] if p + 1 < tiles else after_im)
        o_re, o_im = [], []
        for p in range(tiles):
            js = [(j, j % 2, p + j // 2) for j in range(2 * (tiles - p))]
            o_re.append(total(w_re[j] * z_re[h][k] + w_im[j] * z_im[h][k] for j, h, k in js))
            o_im.append(total(w_re[j] * z_im[h][k] - w_im[j] * z_re[h][k] for j, h, k in js))
        return o_re, o_im

    def give_back(oth, send, rx, copy):
        for p in range(0, tiles, 2):
            both = inverse(jnp.concatenate([oth[p], oth[p + 1]], axis=1))
            for k in range(2):
                for n, piece in enumerate(turn_rows(both[:, k * LANES : (k + 1) * LANES], masks_q)):
                    send[4 * (p + k) + n] = piece
        rx[mine] = send[mine]
        for c in others:
            copy(c, row, mine).start()
            copy(c, other, mine).start()
        copy(me, other, mine).start()

    early = row < ndp // 2

    @pl.when(early)
    def _():
        spread_taps()
        spread_grads()
        greet()
        analyse(all_x, rxx, sigx, rigx)
        weigh()
        over_rows(othx, mix_x)
        give_back(othx, mx_send, mx_rx, copy_mx)
        analyse(all_g, rxg, sigg, rigg)
        over_rows(othg, mix_g)
        give_back(othg, mg_send, mg_rx, copy_mg)
        correlate()
        send_taps(list(range(ndp // 2, ndp)) + list(range(ndp // 2)))

    @pl.when(jnp.logical_not(early))
    def _():
        spread_grads()
        spread_taps()
        greet()
        analyse(all_x, rxx, sigx, rigx)
        analyse(all_g, rxg, sigg, rigg)
        correlate()
        send_taps(range(ndp))
        weigh()
        over_rows(othx, mix_x)
        give_back(othx, mx_send, mx_rx, copy_mx)
        over_rows(othg, mix_g)
        give_back(othg, mg_send, mg_rx, copy_mg)

    for whole in (all_mx, all_mg, all_g2):
        whole().wait_recv()
    for whole in (all_x, all_g, all_f, all_mx, all_mg, all_g2):
        whole().wait_send()


def finish(mx, mg, g2, q, k, v, g, out_hbm, gq_hbm, gk_hbm, gv_hbm, gf_hbm, out_v, gq_v, gk_v, gv_v, gf_v, sems):
    length = q.shape[1]
    ql = length // 4
    tiles = mg.shape[0] // 4
    masks_q, masks_f = groups(ql, BF16), groups(ql, F32)

    pairs = ((out_v, out_hbm), (gq_v, gq_hbm), (gk_v, gk_hbm), (gv_v, gv_hbm), (gf_v, gf_hbm))
    for p in range(tiles):
        cols = slice(p * LANES, (p + 1) * LANES)
        mixed, back = [
            jnp.concatenate(turn(*[m[4 * p + n] for n in range(4)], masks_q), axis=0).astype(F32) for m in (mx, mg)
        ]
        out_v[0, :, cols] = (q[0, :, cols].astype(F32) * mixed).astype(BF16)
        gq_v[0, :, cols] = (g[0, :, cols].astype(F32) * mixed).astype(BF16)
        gk_v[0, :, cols] = (v[0, :, cols].astype(F32) * back).astype(BF16)
        gv_v[0, :, cols] = (k[0, :, cols].astype(F32) * back).astype(BF16)
        quads = [g2[4 * p + n].astype(F32) + g2[4 * (tiles + p) + n].astype(F32) for n in range(4)]
        for n, piece in enumerate(turn(*quads, masks_f)):
            gf_v[n * ql : (n + 1) * ql, cols] = piece
        for n, (src, dst) in enumerate(pairs):
            part = (slice(None),) * (len(src.shape) - 1) + (cols,)
            pltpu.make_async_copy(src.at[part], dst.at[part], sems.at[n]).start()
    for n, (src, dst) in enumerate(pairs):
        pltpu.make_async_copy(src, dst, sems.at[n]).wait()


def fused(nctx, ndp, query, key_input, value_input, filter_taps, grad_output):
    length, channels = query.shape[1], query.shape[2]
    ahead, back = block_tables(length)
    vm = pl.BlockSpec(memory_space=pltpu.VMEM)
    hbm = pl.BlockSpec(memory_space=pltpu.HBM)
    ql, tiles = length // 4, nctx // 2
    dma = pltpu.SemaphoreType.DMA
    kept = 2 * (4 * query.size + (4 * nctx + ndp * nctx) * ql * LANES) + 16384
    pieces = pltpu.VMEM((2 * nctx, ql, LANES), BF16)
    spectrum = pltpu.VMEM((tiles, 2 * length, LANES), F32)
    arrived = pl.pallas_call(
        functools.partial(kernel, nctx, ndp),
        out_shape=(
            pieces,
            pieces,
            pltpu.VMEM((ndp * nctx, ql, LANES), BF16),
            pltpu.VMEM(query.shape, BF16),
            pltpu.VMEM(query.shape, BF16),
            pltpu.VMEM(query.shape, BF16),
            pltpu.VMEM(query.shape, BF16),
        ),
        in_specs=[hbm] * 7,
        out_specs=(vm,) * 7,
        scratch_shapes=[
            pltpu.VMEM((length, channels), F32),
            pltpu.VMEM(ahead.shape, BF16),
            pltpu.VMEM(back.shape, BF16),
            pieces,
            pieces,
            pieces,
            pieces,
            pieces,
            pltpu.VMEM((nctx, ql, LANES), BF16),
            spectrum,
            spectrum,
            spectrum,
            spectrum,
            pltpu.VMEM((tiles, 2 * length, 2 * LANES), F32),
            pltpu.VMEM((tiles, 2 * length, LANES), BF16),
            pltpu.VMEM((tiles, 2 * length, LANES), BF16),
            pltpu.VMEM((nctx, 2 * length, LANES), F32),
            pltpu.VMEM((2 * length, nctx // 4 * LANES), BF16),
            pltpu.VMEM((nctx, ql, LANES), BF16),
            pieces,
            pieces,
            pltpu.SemaphoreType.REGULAR,
            dma((7,)),
        ]
        + [dma] * 12,
        compiler_params=pltpu.CompilerParams(
            collective_id=0, has_side_effects=True, vmem_limit_bytes=VMEM_BYTES - kept
        ),
    )(query, key_input, value_input, filter_taps, grad_output, jnp.asarray(ahead), jnp.asarray(back))
    wide = jax.ShapeDtypeStruct(query.shape, BF16)
    return pl.pallas_call(
        finish,
        out_shape=(wide, wide, wide, wide, jax.ShapeDtypeStruct((length, channels), F32)),
        in_specs=[vm] * 7,
        out_specs=(hbm,) * 5,
        scratch_shapes=[pltpu.VMEM(query.shape, BF16)] * 4 + [pltpu.VMEM((length, channels), F32), dma((5,))],
        compiler_params=pltpu.CompilerParams(vmem_limit_bytes=16 * 1024 * 1024),
    )(*arrived)


def build_tables(length):
    padded = 2 * length
    columns = 1
    while columns * columns < padded and length % (2 * columns) == 0:
        columns = columns * 2
    row_count = padded // columns
    col_index = jnp.arange(columns, dtype=jnp.int32)
    row_index = jnp.arange(row_count, dtype=jnp.int32)
    col_angle = (col_index[:, None] * col_index[None, :] % columns).astype(jnp.float32) * (
        2.0 * math.pi / columns
    )
    row_angle = (row_index[:, None] * row_index[None, :] % row_count).astype(jnp.float32) * (
        2.0 * math.pi / row_count
    )
    twist_angle = (row_index[:, None] * col_index[None, :] % padded).astype(jnp.float32) * (
        2.0 * math.pi / padded
    )
    return (
        jnp.cos(col_angle),
        -jnp.sin(col_angle),
        jnp.cos(row_angle),
        -jnp.sin(row_angle),
        jnp.cos(twist_angle),
        -jnp.sin(twist_angle),
        row_count,
        columns,
        padded,
    )


def forward(signal, tables):
    col_real, col_imag, row_real, row_imag, twist_real, twist_imag, row_count, columns, padded = (
        tables
    )
    half_rows = row_count // 2
    blocks = signal.reshape(signal.shape[0], half_rows, columns, signal.shape[2])
    section_real = jnp.einsum("kn,snac->scka", row_real[:, :half_rows], blocks, precision=HIGH)
    section_imag = jnp.einsum("kn,snac->scka", row_imag[:, :half_rows], blocks, precision=HIGH)
    turned_real = section_real * twist_real - section_imag * twist_imag
    turned_imag = section_real * twist_imag + section_imag * twist_real
    spec_real = jnp.einsum("scka,aj->sckj", turned_real, col_real, precision=HIGH) - jnp.einsum(
        "scka,aj->sckj", turned_imag, col_imag, precision=HIGH
    )
    spec_imag = jnp.einsum("scka,aj->sckj", turned_real, col_imag, precision=HIGH) + jnp.einsum(
        "scka,aj->sckj", turned_imag, col_real, precision=HIGH
    )
    return (spec_real, spec_imag)


def inverse(spec, tables):
    col_real, col_imag, row_real, row_imag, twist_real, twist_imag, row_count, columns, padded = (
        tables
    )
    spec_real, spec_imag = spec
    half_rows = row_count // 2
    section_real = jnp.einsum("scka,aj->sckj", spec_real, col_real, precision=HIGH) + jnp.einsum(
        "scka,aj->sckj", spec_imag, col_imag, precision=HIGH
    )
    section_imag = jnp.einsum("scka,aj->sckj", spec_imag, col_real, precision=HIGH) - jnp.einsum(
        "scka,aj->sckj", spec_real, col_imag, precision=HIGH
    )
    turned_real = section_real * twist_real + section_imag * twist_imag
    turned_imag = section_imag * twist_real - section_real * twist_imag
    signal = jnp.einsum(
        "nk,scka->snac", row_real[:half_rows], turned_real, precision=HIGH
    ) + jnp.einsum("nk,scka->snac", row_imag[:half_rows], turned_imag, precision=HIGH)
    return signal.reshape(signal.shape[0], half_rows * columns, signal.shape[3]) * (1.0 / padded)


def times_spec(first, second):
    return (
        first[0] * second[0] - first[1] * second[1],
        first[0] * second[1] + first[1] * second[0],
    )


def times_conj(first, second):
    return (
        first[0] * second[0] + first[1] * second[1],
        first[1] * second[0] - first[0] * second[1],
    )


def local(query, key_input, value_input, filter_taps, grad_output):
    product = (key_input.astype(jnp.float32) * value_input.astype(jnp.float32)).astype(jnp.bfloat16)
    grad_mix = (grad_output.astype(jnp.float32) * query.astype(jnp.float32)).astype(jnp.bfloat16)
    owned_filter = lax.all_to_all(filter_taps, "ctx", split_axis=1, concat_axis=0, tiled=True)
    tables = build_tables(owned_filter.shape[0])
    filter_spec = forward(owned_filter[None], tables)
    local_product = lax.all_to_all(product, "ctx", split_axis=2, concat_axis=1, tiled=True)
    prod_spec = forward(local_product.astype(jnp.float32), tables)
    owned_mixed = inverse(times_spec(filter_spec, prod_spec), tables).astype(jnp.bfloat16)
    owned_mixed, prod_spec = (owned_mixed, prod_spec)
    mixed = lax.all_to_all(owned_mixed, "ctx", split_axis=1, concat_axis=2, tiled=True)
    owned_grad = lax.all_to_all(grad_mix, "ctx", split_axis=2, concat_axis=1, tiled=True)
    grad_spec = forward(owned_grad.astype(jnp.float32), tables)
    owned_back = inverse(times_conj(grad_spec, filter_spec), tables).astype(jnp.bfloat16)
    taps_spec = times_conj(grad_spec, prod_spec)
    owned_back, taps_spec = (
        owned_back,
        (jnp.sum(taps_spec[0], axis=0), jnp.sum(taps_spec[1], axis=0)),
    )
    grad_product = lax.all_to_all(owned_back, "ctx", split_axis=1, concat_axis=2, tiled=True)
    mixed_wide = mixed.astype(jnp.float32)
    back_wide = grad_product.astype(jnp.float32)
    output = (query.astype(jnp.float32) * mixed_wide).astype(jnp.bfloat16)
    grad_query = (grad_output.astype(jnp.float32) * mixed_wide).astype(jnp.bfloat16)
    grad_key = (back_wide * value_input.astype(jnp.float32)).astype(jnp.bfloat16)
    grad_value = (back_wide * key_input.astype(jnp.float32)).astype(jnp.bfloat16)
    local_taps = inverse((taps_spec[0][None], taps_spec[1][None]), tables)[0]
    owned_taps = lax.psum(local_taps, "dp")
    grad_filter = lax.all_to_all(owned_taps, "ctx", split_axis=0, concat_axis=1, tiled=True)
    return (output, grad_query, grad_key, grad_value, grad_filter)


def plan(mesh, query, key_input, value_input, filter_taps, grad_output):
    nctx, ndp = mesh.shape["ctx"], mesh.shape["dp"]
    sequences, length, channels = query.shape
    paired = nctx == 2 * ndp and ndp // 2 == 2
    fits = paired and 2 * channels == nctx * LANES and sequences == 1 and length % 64 == 0 and length <= LANES
    run = functools.partial(fused, nctx, ndp) if fits else local
    return run(query, key_input, value_input, filter_taps, grad_output)


def solution(mesh):
    wide, taps = P("dp", "ctx", None), P("ctx", None)
    return jax.shard_map(
        functools.partial(plan, mesh),
        mesh=mesh,
        in_specs=(wide, wide, wide, taps, wide),
        out_specs=(wide, wide, wide, wide, taps),
        check_vma=False,
    )
```

```python
import functools
import math

import jax
import jax.numpy as jnp
import numpy as np
from jax import lax
from jax.experimental import pallas as pl
from jax.experimental.pallas import tpu as pltpu
from jax.sharding import PartitionSpec as P

HIGH = lax.Precision.HIGHEST
MESH = pl.DeviceIdType.MESH
LANES = 128
VMEM_BYTES = 67043328
F32 = jnp.float32
BF16 = jnp.bfloat16


def block_tables(length):
    odd = 2 * np.arange(length, dtype=np.int64)[:, None] + 1
    angle = (odd * np.arange(length, dtype=np.int64)[None, :] % (4 * length)) * (2.0 * math.pi / (4 * length))
    ahead = np.concatenate([np.cos(angle), -np.sin(angle)], axis=0).astype(np.float32)
    back = ahead.T / np.float32(length)

    def split(table):
        high = jnp.asarray(table).astype(BF16)
        low = (jnp.asarray(table) - high.astype(F32)).astype(BF16)
        return high, low

    with jax.ensure_compile_time_eval():
        ahead_high, ahead_low = split(ahead)
        back_high, back_low = split(back)
        return (
            np.asarray(jnp.concatenate([ahead_high, ahead_low], axis=1)),
            np.asarray(jnp.concatenate([back_high, back_low], axis=1)),
        )


def groups(rows, dtype):
    kind = jnp.int16 if dtype == BF16 else jnp.int32
    lane = lax.broadcasted_iota(kind, (rows, LANES), 1)
    low = lane < LANES // 2
    even = (lane < LANES // 4) | ((lane >= LANES // 2) & (lane < 3 * LANES // 4))
    return low, even


def turn(a, b, c, d, masks):
    low, even = masks

    def halves(first, second):
        turned = pltpu.roll(jnp.where(low, second, first), LANES // 2, 1)
        return jnp.where(low, first, turned), jnp.where(low, turned, second)

    def quarters(first, second):
        return (
            jnp.where(even, first, pltpu.roll(second, LANES // 4, 1)),
            jnp.where(even, pltpu.roll(first, LANES - LANES // 4, 1), second),
        )

    (a, c), (b, d) = halves(a, c), halves(b, d)
    return quarters(a, b) + quarters(c, d)


def turn_rows(tile, masks):
    rows = tile.shape[0] // 4
    return turn(*[tile[n * rows : (n + 1) * rows] for n in range(4)], masks)


def flip(index, mask):
    out, bit = index, 1
    while bit <= mask:
        if mask & bit:
            out = out + bit * (1 - 2 * lax.rem(index // bit, 2))
        bit = 2 * bit
    return out


def total(terms):
    out = None
    for term in terms:
        out = term if out is None else out + term
    return out


def kernel(
    nctx,
    ndp,
    q_hbm,
    k_hbm,
    v_hbm,
    f_hbm,
    g_hbm,
    ahead_hbm,
    back_hbm,
    g2_rx,
    out_v,
    gq_v,
    gk_v,
    gv_v,
    mx_rx,
    mg_rx,
    qv,
    kv,
    vv,
    gv,
    fv,
    ahead_v,
    back_v,
    sendx,
    sendg,
    sendf,
    rxx,
    rxg,
    rxf,
    sigx,
    sigg,
    rigx,
    rigg,
    wei,
    othx,
    othg,
    acc,
    gfs,
    g2_send,
    mx_send,
    mg_send,
    known,
    load_sem,
    x_ssem,
    x_rsem,
    g_ssem,
    g_rsem,
    f_ssem,
    f_rsem,
    g2_ssem,
    g2_rsem,
    own_rsem,
    fwd_ssem,
    fwd_rsem,
    mx_ssem,
    mx_rsem,
    mg_ssem,
    mg_rsem,
):
    me = lax.axis_index("ctx")
    row = lax.axis_index("dp")
    length = qv.shape[1]
    ql = length // 4
    tiles = nctx // 2
    part = lax.rem(row, 2)
    base = row - part
    other = base + 1 - part
    mine = 2 * me + part
    slot = row * nctx + me
    early = row < ndp // 2

    pairs = ((k_hbm, kv), (v_hbm, vv), (g_hbm, gv), (q_hbm, qv), (f_hbm, fv), (ahead_hbm, ahead_v), (back_hbm, back_v))
    loads = [pltpu.make_async_copy(src, dst, load_sem.at[n]) for n, (src, dst) in enumerate(pairs)]
    def at(ctx, dp):
        return {"ctx": ctx, "dp": dp}

    inner = jnp.logical_and(part == 1, row + 1 < ndp)
    outer = jnp.logical_and(part == 0, row > 0)
    across = row + 2 * part - 1
    border = jnp.logical_or(inner, outer)
    barrier = pltpu.get_barrier_semaphore()
    pals = [(other, me)] + [(r, flip(me, o)) for o in range(1, nctx) for r in (row, other)]
    for r, c in reversed(pals):
        pl.semaphore_signal(barrier, inc=1, device_id=at(c, r), device_id_type=MESH)

    @pl.when(border)
    def _():
        pl.semaphore_signal(barrier, inc=1, device_id=at(me, across), device_id_type=MESH)

    for p in range(tiles):
        cols = slice(p * LANES, (p + 1) * LANES)
        for n, (src, dst) in enumerate(pairs[:2]):
            pltpu.make_async_copy(src.at[:, :, cols], dst.at[:, :, cols], load_sem.at[n]).start()
    for load in loads[2:]:
        load.start()
    masks_q = groups(ql, BF16)

    def prepare(a_ref, b_ref, into):
        for p in range(tiles):
            cols = slice(p * LANES, (p + 1) * LANES)
            tile = (a_ref[0, :, cols].astype(F32) * b_ref[0, :, cols].astype(F32)).astype(BF16)
            for n, piece in enumerate(turn_rows(tile, masks_q)):
                into[4 * p + n] = piece

    for load in loads[:2]:
        load.wait()
    prepare(kv, vv, sendx)
    rxx[mine] = sendx[mine]
    pl.semaphore_wait(barrier, len(pals) + jnp.where(border, 1, 0))

    def remote(src, dst, ssem, rsem, ctx, dp):
        return pltpu.make_async_remote_copy(
            src_ref=src, dst_ref=dst, send_sem=ssem, recv_sem=rsem, device_id=at(ctx, dp), device_id_type=MESH
        )

    def tile_copy(src, dst, ssem, rsem):
        def copy(ctx, dp, into):
            to = 2 * ctx + lax.rem(dp, 2)
            return remote(src.at[to], dst.at[into], ssem, rsem, ctx, dp)

        def whole():
            every = pl.ds(0, len(pals))
            return remote(src.at[every], dst.at[every], ssem, rsem, me, other)

        return copy, whole

    copy_x, all_x = tile_copy(sendx, rxx, x_ssem, x_rsem)
    copy_g, all_g = tile_copy(sendg, rxg, g_ssem, g_rsem)
    copy_mx, all_mx = tile_copy(mx_send, mx_rx, mx_ssem, mx_rsem)
    copy_mg, all_mg = tile_copy(mg_send, mg_rx, mg_ssem, mg_rsem)

    def copy_f(ctx, into):
        return remote(sendf.at[2 * ctx + part], rxf.at[into], f_ssem, f_rsem, ctx, row)

    def copy_g2(ctx, dp, rsem):
        return remote(g2_send.at[ctx], g2_rx.at[slot], g2_ssem, rsem, ctx, dp)

    def wait_g2(rsem, count):
        every = pl.ds(0, count)
        return remote(g2_rx.at[every], g2_rx.at[every], g2_ssem, rsem, me, other)

    def forward(dp):
        block = pl.ds(pl.multiple_of(dp * nctx, nctx), nctx)
        return remote(g2_rx.at[block], g2_rx.at[block], fwd_ssem, fwd_rsem, me, other)

    def all_f():
        every = pl.ds(0, nctx - 1)
        return remote(sendf.at[every], rxf.at[every], f_ssem, f_rsem, me, other)

    for r, c in pals:
        copy_x(c, r, mine).start()

    @pl.when(border)
    def _():
        pl.semaphore_signal(known, inc=1, device_id=at(me, across), device_id_type=MESH)

    others = [k + jnp.where(me <= k, 1, 0) for k in range(nctx - 1)]

    def spread_grads():
        for load in loads[2:4]:
            load.wait()
        prepare(gv, qv, sendg)
        rxg[mine] = sendg[mine]
        for r, c in pals:
            copy_g(c, r, mine).start()

    def spread_taps():
        loads[4].wait()
        for p in range(tiles):
            for n, piece in enumerate(turn_rows(fv[:, p * LANES : (p + 1) * LANES].astype(BF16), masks_q)):
                sendf[4 * p + n] = piece
        rxf[me] = sendf[mine]
        for o in range(1, nctx):
            copy_f(flip(me, o), me).start()

    def greet():
        for load in loads[5:]:
            load.wait()
        pl.semaphore_wait(known, 1)

        @pl.when(border)
        def _():
            pl.semaphore_signal(known, inc=1, device_id=at(me, other), device_id_type=MESH)

    def transform(z):
        return jnp.dot(ahead_v[...], jnp.concatenate([z, z], axis=0), preferred_element_type=F32)

    def analyse(whole, rx, sig, rig=None):
        whole().wait_recv()
        z = [jnp.concatenate(turn(*[rx[4 * p + n] for n in range(4)], masks_q), axis=0) for p in range(tiles)]
        for p in range(0, tiles, 2):
            spec = transform(jnp.concatenate(z[p : p + 2], axis=1))
            for k in range(2):
                half = spec[:, k * LANES : (k + 1) * LANES]
                sig[p + k] = half
                if rig is not None:
                    rig[p + k] = pltpu.roll(half, LANES // 2, 1)

    def swap_grads():
        for p in range(tiles):
            rigg[p] = pltpu.roll(sigg[p], LANES // 2, 1)

    low, _ = groups(8, F32)
    parity = lax.rem(lax.broadcasted_iota(jnp.int32, (8, LANES), 0), 2)
    alt = jnp.where(parity == 0, 1.0, -1.0).astype(F32)
    zero = jnp.zeros((8, LANES), F32)

    def windows(re, im):
        x_re = [zero] + [sigx[p, re, :] for p in range(tiles)]
        x_im = [zero] + [sigx[p, im, :] for p in range(tiles)]
        r_re = [zero] + [rigx[p, re, :] for p in range(tiles)]
        r_im = [zero] + [rigx[p, im, :] for p in range(tiles)]
        z_re, z_im = [[], []], [[], []]
        for p in range(tiles):
            before_re, before_im = jnp.where(low, r_re[p], r_re[p + 1]), jnp.where(low, r_im[p], r_im[p + 1])
            z_re[0].append(x_re[p + 1] - alt * before_im)
            z_im[0].append(x_im[p + 1] + alt * before_re)
            z_re[1].append(before_re - alt * x_im[p] if p else before_re)
            z_im[1].append(before_im + alt * x_re[p] if p else before_im)
        return z_re, z_im

    def rows_at(i, start):
        return pl.ds(pl.multiple_of(start + i * 8, 8), 8)

    def correlate():
        @pl.loop(0, length // 8, unroll=2)
        def _(i):
            re, im = rows_at(i, 0), rows_at(i, length)
            z_re, z_im = windows(re, im)
            g_re = [sigg[p, re, :] for p in range(tiles)]
            g_im = [sigg[p, im, :] for p in range(tiles)]
            for j in range(nctx):
                b_re, b_im = z_re[j % 2], z_im[j % 2]
                ms = [(m, m - j // 2) for m in range(j // 2, tiles)]
                acc[j, re, :] = total(g_re[m] * b_re[k] + g_im[m] * b_im[k] for m, k in ms)
                acc[j, im, :] = total(g_im[m] * b_re[k] - g_re[m] * b_im[k] for m, k in ms)

        low_f, even_f = groups(64, F32)

        def swing(here, there):
            return pltpu.roll(jnp.where(low_f, here, there), LANES // 2, 1)

        chunks = [(n, slice(m, m + 64)) for m in range(0, 2 * length, 64) for n in range(nctx // 4)]
        for n, rows in chunks:
            for k in (0, 2):
                a, b = acc[4 * n + k, rows, :], acc[4 * n + k + 1, rows, :]
                moved = pltpu.roll(jnp.where(even_f, b, a), LANES // 4, 1)
                acc[4 * n + k, rows, :] = jnp.where(even_f, a, b) + moved
        for n, rows in chunks:
            a, b = acc[4 * n, rows, :], acc[4 * n + 2, rows, :]
            gfs[rows, n * LANES : (n + 1) * LANES] = (jnp.where(low_f, a, b) + swing(b, a)).astype(BF16)

    def inverse(high):
        return jnp.dot(back_v[...], jnp.concatenate([high, high], axis=0), preferred_element_type=F32).astype(BF16)

    def send_taps(dp, rsem, here=False):
        for c in others:
            copy_g2(c, dp, rsem).start()
        if not here:
            copy_g2(me, dp, rsem).start()

    def send_pair(index):
        @pl.when(part == index)
        def _():
            send_taps(row, g2_rsem, True)

        @pl.when(part != index)
        def _():
            send_taps(other, g2_rsem)

    def finish_taps():
        taps = inverse(gfs[...])
        for n in range(nctx // 4):
            for m, piece in enumerate(turn_rows(taps[:, n * LANES : (n + 1) * LANES], masks_q)):
                g2_send[4 * n + m] = piece
        g2_rx[slot] = g2_send[me]

    def weigh():
        all_f().wait_recv()
        low_q, even_q = masks_q
        z = []
        for c in range(nctx):
            fa = rxf[c]
            turned = pltpu.roll(fa, LANES // 2, 1)
            pieces = []
            for half in (jnp.where(low_q, fa, turned), jnp.where(low_q, turned, fa)):
                pieces.append(jnp.where(even_q, half, pltpu.roll(half, LANES // 4, 1)))
                pieces.append(jnp.where(even_q, pltpu.roll(half, LANES - LANES // 4, 1), half))
            z.append(jnp.concatenate(pieces, axis=0))
        for p in range(tiles):
            wei[p] = transform(jnp.concatenate(z[2 * p : 2 * p + 2], axis=1))

    def weights(re, im):
        return [[wei[j // 2, rows, pl.ds((j % 2) * LANES, LANES)] for j in range(nctx)] for rows in (re, im)]

    def over_rows(oth, halves):
        @pl.loop(0, length // 16)
        def _(i):
            outs = [halves(rows_at(2 * i + k, 0), rows_at(2 * i + k, length)) for k in range(2)]
            for p in range(tiles):
                for n, start in enumerate((0, length)):
                    rows = pl.ds(pl.multiple_of(start + i * 16, 16), 16)
                    oth[p, rows, :] = jnp.concatenate([outs[0][n][p], outs[1][n][p]], axis=0).astype(BF16)

    def mix_x(re, im):
        w_re, w_im = weights(re, im)
        z_re, z_im = windows(re, im)
        o_re, o_im = [], []
        for p in range(tiles):
            js = [(j, j % 2, p - j // 2) for j in range(2 * p + 2)]
            o_re.append(total(w_re[j] * z_re[h][k] - w_im[j] * z_im[h][k] for j, h, k in js))
            o_im.append(total(w_re[j] * z_im[h][k] + w_im[j] * z_re[h][k] for j, h, k in js))
        return o_re, o_im

    def mix_g(re, im):
        w_re, w_im = weights(re, im)
        g_re = [sigg[p, re, :] for p in range(tiles)]
        g_im = [sigg[p, im, :] for p in range(tiles)]
        r_re = [rigg[p, re, :] for p in range(tiles)] + [zero]
        r_im = [rigg[p, im, :] for p in range(tiles)] + [zero]
        z_re, z_im = [[], []], [[], []]
        for p in range(tiles):
            after_re, after_im = jnp.where(low, r_re[p], r_re[p + 1]), jnp.where(low, r_im[p], r_im[p + 1])
            z_re[0].append(g_re[p] + alt * after_im)
            z_im[0].append(g_im[p] - alt * after_re)
            z_re[1].append(after_re + alt * g_im[p + 1] if p + 1 < tiles else after_re)
            z_im[1].append(after_im - alt * g_re[p + 1] if p + 1 < tiles else after_im)
        o_re, o_im = [], []
        for p in range(tiles):
            js = [(j, j % 2, p + j // 2) for j in range(2 * (tiles - p))]
            o_re.append(total(w_re[j] * z_re[h][k] + w_im[j] * z_im[h][k] for j, h, k in js))
            o_im.append(total(w_re[j] * z_im[h][k] - w_im[j] * z_re[h][k] for j, h, k in js))
        return o_re, o_im

    def give_back(oth, send, rx, copy):
        wide = [inverse(jnp.concatenate([oth[p], oth[p + 1]], axis=1)) for p in range(0, tiles, 2)]
        for p in range(tiles):
            for n, piece in enumerate(turn_rows(wide[p // 2][:, p % 2 * LANES : (p % 2 + 1) * LANES], masks_q)):
                send[4 * p + n] = piece
        rx[mine] = send[mine]
        for c in others:
            copy(c, row, mine).start()
            copy(c, other, mine).start()
        copy(me, other, mine).start()

    @pl.when(early)
    def _():
        spread_taps()
        spread_grads()
        greet()
        analyse(all_x, rxx, sigx, rigx)
        weigh()
        over_rows(othx, mix_x)
        give_back(othx, mx_send, mx_rx, copy_mx)
        analyse(all_g, rxg, sigg, rigg)
        over_rows(othg, mix_g)
        give_back(othg, mg_send, mg_rx, copy_mg)
        correlate()
        finish_taps()
        send_pair(0)
        for dp in range(ndp // 2, ndp):
            send_taps(dp, g2_rsem)
        send_pair(1)

    @pl.when(jnp.logical_not(early))
    def _():
        spread_grads()
        spread_taps()
        greet()
        analyse(all_x, rxx, sigx, rigx)
        analyse(all_g, rxg, sigg)
        correlate()
        finish_taps()
        for dp in range(ndp // 2):
            send_taps(dp, g2_rsem)
        send_taps(row, own_rsem, True)
        weigh()
        swap_grads()
        over_rows(othx, mix_x)
        give_back(othx, mx_send, mx_rx, copy_mx)
        over_rows(othg, mix_g)
        give_back(othg, mg_send, mg_rx, copy_mg)
        wait_g2(own_rsem, nctx - 1).wait_recv()
        forward(row).start()

    def gate(rx, first, first_out, second, second_out):
        for p in range(tiles):
            cols = slice(p * LANES, (p + 1) * LANES)
            value = jnp.concatenate(turn(*[rx[4 * p + n] for n in range(4)], masks_q), axis=0).astype(F32)
            first_out[0, :, cols] = (first[0, :, cols].astype(F32) * value).astype(BF16)
            second_out[0, :, cols] = (second[0, :, cols].astype(F32) * value).astype(BF16)

    all_mx().wait_recv()
    gate(mx_rx, qv, out_v, gv, gq_v)
    all_mg().wait_recv()
    gate(mg_rx, vv, gk_v, kv, gv_v)

    @pl.when(early)
    def _():
        wait_g2(g2_rsem, ndp * nctx - 1).wait_recv()
        wait_g2(g2_rsem, ndp * nctx - 1).wait_send()

    @pl.when(jnp.logical_not(early))
    def _():
        wait_g2(g2_rsem, ndp // 2 * nctx).wait_recv()
        wait_g2(fwd_rsem, nctx).wait_recv()
        forward(row).wait_send()
        wait_g2(g2_rsem, (ndp // 2 + 1) * nctx - 1).wait_send()

    for whole in (all_x, all_g, all_f, all_mx, all_mg):
        whole().wait_send()


def finish(g2, out, gq, gk, gv, out_hbm, gq_hbm, gk_hbm, gv_hbm, gf_hbm, gf_v, sems):
    length, channels = gf_v.shape
    ql, tiles = length // 4, channels // LANES
    copies = []
    for n, (src, dst) in enumerate(((out, out_hbm), (gq, gq_hbm), (gk, gk_hbm), (gv, gv_hbm), (gf_v, gf_hbm))):
        copies.append(pltpu.make_async_copy(src, dst, sems.at[n]))
    for copy in copies[:4]:
        copy.start()
    masks_f = groups(ql, F32)
    for p in range(tiles):
        cols = slice(p * LANES, (p + 1) * LANES)
        quads = [
            total(g2[2 * tiles * (2 * q + n % 2) + 2 * p + n // 2].astype(F32) for q in range(g2.shape[0] // (4 * tiles)))
            for n in range(4)
        ]
        for n, piece in enumerate(turn(*quads, masks_f)):
            gf_v[n * ql : (n + 1) * ql, cols] = piece
        pltpu.make_async_copy(gf_v.at[:, cols], gf_hbm.at[:, cols], sems.at[4]).start()
    for copy in copies:
        copy.wait()


def fused(nctx, ndp, query, key_input, value_input, filter_taps, grad_output):
    length, channels = query.shape[1], query.shape[2]
    ahead, back = block_tables(length)
    vm = pl.BlockSpec(memory_space=pltpu.VMEM)
    hbm = pl.BlockSpec(memory_space=pltpu.HBM)
    ql, tiles = length // 4, nctx // 2
    dma = pltpu.SemaphoreType.DMA
    kept = 2 * (4 * query.size + ndp * nctx * ql * LANES) + 16384
    pieces = pltpu.VMEM((2 * nctx, ql, LANES), BF16)
    spectrum = pltpu.VMEM((tiles, 2 * length, LANES), F32)
    arrived = pl.pallas_call(
        functools.partial(kernel, nctx, ndp),
        out_shape=(pltpu.VMEM((ndp * nctx, ql, LANES), BF16),) + (pltpu.VMEM(query.shape, BF16),) * 4,
        in_specs=[hbm] * 7,
        out_specs=(vm,) * 5,
        scratch_shapes=[
            pieces,
            pieces,
            pltpu.VMEM(query.shape, BF16),
            pltpu.VMEM(query.shape, BF16),
            pltpu.VMEM(query.shape, BF16),
            pltpu.VMEM(query.shape, BF16),
            pltpu.VMEM((length, channels), F32),
            pltpu.VMEM(ahead.shape, BF16),
            pltpu.VMEM(back.shape, BF16),
            pieces,
            pieces,
            pieces,
            pieces,
            pieces,
            pltpu.VMEM((nctx, ql, LANES), BF16),
            spectrum,
            spectrum,
            spectrum,
            spectrum,
            pltpu.VMEM((tiles, 2 * length, 2 * LANES), F32),
            pltpu.VMEM((tiles, 2 * length, LANES), BF16),
            pltpu.VMEM((tiles, 2 * length, LANES), BF16),
            pltpu.VMEM((nctx, 2 * length, LANES), F32),
            pltpu.VMEM((2 * length, nctx // 4 * LANES), BF16),
            pltpu.VMEM((nctx, ql, LANES), BF16),
            pieces,
            pieces,
            pltpu.SemaphoreType.REGULAR,
            dma((7,)),
        ]
        + [dma] * 15,
        compiler_params=pltpu.CompilerParams(
            collective_id=0, has_side_effects=True, vmem_limit_bytes=VMEM_BYTES - kept
        ),
    )(query, key_input, value_input, filter_taps, grad_output, jnp.asarray(ahead), jnp.asarray(back))
    wide = jax.ShapeDtypeStruct(query.shape, BF16)
    return pl.pallas_call(
        finish,
        out_shape=(wide, wide, wide, wide, jax.ShapeDtypeStruct((length, channels), F32)),
        in_specs=[vm] * 5,
        out_specs=(hbm,) * 5,
        scratch_shapes=[pltpu.VMEM((length, channels), F32), dma((5,))],
        compiler_params=pltpu.CompilerParams(vmem_limit_bytes=16 * 1024 * 1024),
    )(*arrived)


def build_tables(length):
    padded = 2 * length
    columns = 1
    while columns * columns < padded and length % (2 * columns) == 0:
        columns = columns * 2
    row_count = padded // columns
    col_index = jnp.arange(columns, dtype=jnp.int32)
    row_index = jnp.arange(row_count, dtype=jnp.int32)
    col_angle = (col_index[:, None] * col_index[None, :] % columns).astype(jnp.float32) * (
        2.0 * math.pi / columns
    )
    row_angle = (row_index[:, None] * row_index[None, :] % row_count).astype(jnp.float32) * (
        2.0 * math.pi / row_count
    )
    twist_angle = (row_index[:, None] * col_index[None, :] % padded).astype(jnp.float32) * (
        2.0 * math.pi / padded
    )
    return (
        jnp.cos(col_angle),
        -jnp.sin(col_angle),
        jnp.cos(row_angle),
        -jnp.sin(row_angle),
        jnp.cos(twist_angle),
        -jnp.sin(twist_angle),
        row_count,
        columns,
        padded,
    )


def forward(signal, tables):
    col_real, col_imag, row_real, row_imag, twist_real, twist_imag, row_count, columns, padded = (
        tables
    )
    half_rows = row_count // 2
    blocks = signal.reshape(signal.shape[0], half_rows, columns, signal.shape[2])
    section_real = jnp.einsum("kn,snac->scka", row_real[:, :half_rows], blocks, precision=HIGH)
    section_imag = jnp.einsum("kn,snac->scka", row_imag[:, :half_rows], blocks, precision=HIGH)
    turned_real = section_real * twist_real - section_imag * twist_imag
    turned_imag = section_real * twist_imag + section_imag * twist_real
    spec_real = jnp.einsum("scka,aj->sckj", turned_real, col_real, precision=HIGH) - jnp.einsum(
        "scka,aj->sckj", turned_imag, col_imag, precision=HIGH
    )
    spec_imag = jnp.einsum("scka,aj->sckj", turned_real, col_imag, precision=HIGH) + jnp.einsum(
        "scka,aj->sckj", turned_imag, col_real, precision=HIGH
    )
    return (spec_real, spec_imag)


def inverse(spec, tables):
    col_real, col_imag, row_real, row_imag, twist_real, twist_imag, row_count, columns, padded = (
        tables
    )
    spec_real, spec_imag = spec
    half_rows = row_count // 2
    section_real = jnp.einsum("scka,aj->sckj", spec_real, col_real, precision=HIGH) + jnp.einsum(
        "scka,aj->sckj", spec_imag, col_imag, precision=HIGH
    )
    section_imag = jnp.einsum("scka,aj->sckj", spec_imag, col_real, precision=HIGH) - jnp.einsum(
        "scka,aj->sckj", spec_real, col_imag, precision=HIGH
    )
    turned_real = section_real * twist_real + section_imag * twist_imag
    turned_imag = section_imag * twist_real - section_real * twist_imag
    signal = jnp.einsum(
        "nk,scka->snac", row_real[:half_rows], turned_real, precision=HIGH
    ) + jnp.einsum("nk,scka->snac", row_imag[:half_rows], turned_imag, precision=HIGH)
    return signal.reshape(signal.shape[0], half_rows * columns, signal.shape[3]) * (1.0 / padded)


def times_spec(first, second):
    return (
        first[0] * second[0] - first[1] * second[1],
        first[0] * second[1] + first[1] * second[0],
    )


def times_conj(first, second):
    return (
        first[0] * second[0] + first[1] * second[1],
        first[1] * second[0] - first[0] * second[1],
    )


def local(query, key_input, value_input, filter_taps, grad_output):
    product = (key_input.astype(jnp.float32) * value_input.astype(jnp.float32)).astype(jnp.bfloat16)
    grad_mix = (grad_output.astype(jnp.float32) * query.astype(jnp.float32)).astype(jnp.bfloat16)
    owned_filter = lax.all_to_all(filter_taps, "ctx", split_axis=1, concat_axis=0, tiled=True)
    tables = build_tables(owned_filter.shape[0])
    filter_spec = forward(owned_filter[None], tables)
    local_product = lax.all_to_all(product, "ctx", split_axis=2, concat_axis=1, tiled=True)
    prod_spec = forward(local_product.astype(jnp.float32), tables)
    owned_mixed = inverse(times_spec(filter_spec, prod_spec), tables).astype(jnp.bfloat16)
    owned_mixed, prod_spec = (owned_mixed, prod_spec)
    mixed = lax.all_to_all(owned_mixed, "ctx", split_axis=1, concat_axis=2, tiled=True)
    owned_grad = lax.all_to_all(grad_mix, "ctx", split_axis=2, concat_axis=1, tiled=True)
    grad_spec = forward(owned_grad.astype(jnp.float32), tables)
    owned_back = inverse(times_conj(grad_spec, filter_spec), tables).astype(jnp.bfloat16)
    taps_spec = times_conj(grad_spec, prod_spec)
    owned_back, taps_spec = (
        owned_back,
        (jnp.sum(taps_spec[0], axis=0), jnp.sum(taps_spec[1], axis=0)),
    )
    grad_product = lax.all_to_all(owned_back, "ctx", split_axis=1, concat_axis=2, tiled=True)
    mixed_wide = mixed.astype(jnp.float32)
    back_wide = grad_product.astype(jnp.float32)
    output = (query.astype(jnp.float32) * mixed_wide).astype(jnp.bfloat16)
    grad_query = (grad_output.astype(jnp.float32) * mixed_wide).astype(jnp.bfloat16)
    grad_key = (back_wide * value_input.astype(jnp.float32)).astype(jnp.bfloat16)
    grad_value = (back_wide * key_input.astype(jnp.float32)).astype(jnp.bfloat16)
    local_taps = inverse((taps_spec[0][None], taps_spec[1][None]), tables)[0]
    owned_taps = lax.psum(local_taps, "dp")
    grad_filter = lax.all_to_all(owned_taps, "ctx", split_axis=0, concat_axis=1, tiled=True)
    return (output, grad_query, grad_key, grad_value, grad_filter)


def plan(mesh, query, key_input, value_input, filter_taps, grad_output):
    nctx, ndp = mesh.shape["ctx"], mesh.shape["dp"]
    sequences, length, channels = query.shape
    paired = nctx == 2 * ndp and ndp // 2 == 2
    fits = paired and 2 * channels == nctx * LANES and sequences == 1 and length % 64 == 0 and length <= LANES
    run = functools.partial(fused, nctx, ndp) if fits else local
    return run(query, key_input, value_input, filter_taps, grad_output)


def solution(mesh):
    wide, taps = P("dp", "ctx", None), P("ctx", None)
    return jax.shard_map(
        functools.partial(plan, mesh),
        mesh=mesh,
        in_specs=(wide, wide, wide, taps, wide),
        out_specs=(wide, wide, wide, wide, taps),
        check_vma=False,
    )
```

```python
import functools
import math

import jax
import jax.numpy as jnp
import numpy as np
from jax import lax
from jax.experimental import pallas as pl
from jax.experimental.pallas import tpu as pltpu
from jax.sharding import PartitionSpec as P

HIGH = lax.Precision.HIGHEST
MESH = pl.DeviceIdType.MESH
LANES = 128
VMEM_BYTES = 67043328
F32 = jnp.float32
BF16 = jnp.bfloat16


def block_tables(length):
    odd = 2 * np.arange(length, dtype=np.int64)[:, None] + 1
    angle = (odd * np.arange(length, dtype=np.int64)[None, :] % (4 * length)) * (2.0 * math.pi / (4 * length))
    ahead = np.concatenate([np.cos(angle), -np.sin(angle)], axis=0).astype(np.float32)
    back = ahead.T / np.float32(length)

    def split(table):
        high = jnp.asarray(table).astype(BF16)
        low = (jnp.asarray(table) - high.astype(F32)).astype(BF16)
        return high, low

    with jax.ensure_compile_time_eval():
        ahead_high, ahead_low = split(ahead)
        back_high, _ = split(back)
        return (
            np.asarray(jnp.concatenate([ahead_high, ahead_low], axis=1)),
            np.asarray(back_high),
        )


def groups(rows, dtype):
    kind = jnp.int16 if dtype == BF16 else jnp.int32
    lane = lax.broadcasted_iota(kind, (rows, LANES), 1)
    low = lane < LANES // 2
    even = (lane < LANES // 4) | ((lane >= LANES // 2) & (lane < 3 * LANES // 4))
    return low, even


def turn(a, b, c, d, masks):
    low, even = masks

    def halves(first, second):
        turned = pltpu.roll(jnp.where(low, second, first), LANES // 2, 1)
        return jnp.where(low, first, turned), jnp.where(low, turned, second)

    def quarters(first, second):
        return (
            jnp.where(even, first, pltpu.roll(second, LANES // 4, 1)),
            jnp.where(even, pltpu.roll(first, LANES - LANES // 4, 1), second),
        )

    (a, c), (b, d) = halves(a, c), halves(b, d)
    return quarters(a, b) + quarters(c, d)


def turn_rows(tile, masks):
    rows = tile.shape[0] // 4
    return turn(*[tile[n * rows : (n + 1) * rows] for n in range(4)], masks)


def flip(index, mask):
    out, bit = index, 1
    while bit <= mask:
        if mask & bit:
            out = out + bit * (1 - 2 * lax.rem(index // bit, 2))
        bit = 2 * bit
    return out


def total(terms):
    out = None
    for term in terms:
        out = term if out is None else out + term
    return out


def kernel(
    nctx,
    ndp,
    q_hbm,
    k_hbm,
    v_hbm,
    f_hbm,
    g_hbm,
    ahead_hbm,
    back_hbm,
    g2_rx,
    out_v,
    gq_v,
    gk_v,
    gv_v,
    mx_rx,
    mg_rx,
    qv,
    kv,
    vv,
    gv,
    fv,
    ahead_v,
    back_v,
    sendx,
    sendg,
    sendf,
    rxx,
    rxg,
    rxf,
    sigx,
    sigg,
    rigx,
    rigg,
    wei,
    othx,
    othg,
    acc,
    gfs,
    g2_send,
    mx_send,
    mg_send,
    known,
    load_sem,
    x_ssem,
    x_rsem,
    g_ssem,
    g_rsem,
    f_ssem,
    f_rsem,
    g2_ssem,
    g2_rsem,
    own_rsem,
    fwd_ssem,
    fwd_rsem,
    mx_ssem,
    mx_rsem,
    mg_ssem,
    mg_rsem,
):
    me = lax.axis_index("ctx")
    row = lax.axis_index("dp")
    length = qv.shape[1]
    ql = length // 4
    tiles = nctx // 2
    part = lax.rem(row, 2)
    base = row - part
    other = base + 1 - part
    mine = 2 * me + part
    slot = row * nctx + me
    early = row < ndp // 2

    pairs = ((k_hbm, kv), (v_hbm, vv), (g_hbm, gv), (q_hbm, qv), (f_hbm, fv), (ahead_hbm, ahead_v), (back_hbm, back_v))
    loads = [pltpu.make_async_copy(src, dst, load_sem.at[n]) for n, (src, dst) in enumerate(pairs)]
    def at(ctx, dp):
        return {"ctx": ctx, "dp": dp}

    inner = jnp.logical_and(part == 1, row + 1 < ndp)
    outer = jnp.logical_and(part == 0, row > 0)
    across = row + 2 * part - 1
    border = jnp.logical_or(inner, outer)
    barrier = pltpu.get_barrier_semaphore()
    pals = [(other, me)] + [(r, flip(me, o)) for o in range(1, nctx) for r in (row, other)]
    for r, c in reversed(pals):
        pl.semaphore_signal(barrier, inc=1, device_id=at(c, r), device_id_type=MESH)

    @pl.when(border)
    def _():
        pl.semaphore_signal(barrier, inc=1, device_id=at(me, across), device_id_type=MESH)

    for p in range(tiles):
        cols = slice(p * LANES, (p + 1) * LANES)
        for n, (src, dst) in enumerate(pairs[:2]):
            pltpu.make_async_copy(src.at[:, :, cols], dst.at[:, :, cols], load_sem.at[n]).start()
    for load in loads[2:]:
        load.start()
    masks_q, masks_w = groups(ql, BF16), groups(length, BF16)

    def prepare(a_ref, b_ref, into):
        for p in range(tiles):
            cols = slice(p * LANES, (p + 1) * LANES)
            tile = (a_ref[0, :, cols].astype(F32) * b_ref[0, :, cols].astype(F32)).astype(BF16)
            for n, piece in enumerate(turn_rows(tile, masks_q)):
                into[4 * p + n] = piece

    for load in loads[:2]:
        load.wait()
    prepare(kv, vv, sendx)
    rxx[mine] = sendx[mine]
    pl.semaphore_wait(barrier, len(pals) + jnp.where(border, 1, 0))

    def remote(src, dst, ssem, rsem, ctx, dp):
        return pltpu.make_async_remote_copy(
            src_ref=src, dst_ref=dst, send_sem=ssem, recv_sem=rsem, device_id=at(ctx, dp), device_id_type=MESH
        )

    def tile_copy(src, dst, ssem, rsem):
        def copy(ctx, dp, into):
            to = 2 * ctx + lax.rem(dp, 2)
            return remote(src.at[to], dst.at[into], ssem, rsem, ctx, dp)

        def whole():
            every = pl.ds(0, len(pals))
            return remote(src.at[every], dst.at[every], ssem, rsem, me, other)

        return copy, whole

    copy_x, all_x = tile_copy(sendx, rxx, x_ssem, x_rsem)
    copy_g, all_g = tile_copy(sendg, rxg, g_ssem, g_rsem)
    copy_mx, all_mx = tile_copy(mx_send, mx_rx, mx_ssem, mx_rsem)
    copy_mg, all_mg = tile_copy(mg_send, mg_rx, mg_ssem, mg_rsem)

    def copy_f(ctx, into):
        return remote(sendf.at[2 * ctx + part], rxf.at[into], f_ssem, f_rsem, ctx, row)

    def copy_g2(ctx, dp, rsem):
        return remote(g2_send.at[ctx], g2_rx.at[slot], g2_ssem, rsem, ctx, dp)

    def wait_g2(rsem, count):
        every = pl.ds(0, count)
        return remote(g2_rx.at[every], g2_rx.at[every], g2_ssem, rsem, me, other)

    def forward(dp):
        block = pl.ds(pl.multiple_of(dp * nctx, nctx), nctx)
        return remote(g2_rx.at[block], g2_rx.at[block], fwd_ssem, fwd_rsem, me, other)

    def all_f():
        every = pl.ds(0, nctx - 1)
        return remote(sendf.at[every], rxf.at[every], f_ssem, f_rsem, me, other)

    for r, c in pals:
        copy_x(c, r, mine).start()

    @pl.when(border)
    def _():
        pl.semaphore_signal(known, inc=1, device_id=at(me, across), device_id_type=MESH)

    others = [k + jnp.where(me <= k, 1, 0) for k in range(nctx - 1)]

    def spread_grads():
        for load in loads[2:4]:
            load.wait()
        prepare(gv, qv, sendg)
        rxg[mine] = sendg[mine]
        for r, c in pals:
            copy_g(c, r, mine).start()

    def spread_taps():
        loads[4].wait()
        for p in range(tiles):
            for n, piece in enumerate(turn_rows(fv[:, p * LANES : (p + 1) * LANES].astype(BF16), masks_q)):
                sendf[4 * p + n] = piece
        rxf[me] = sendf[mine]
        for o in range(1, nctx):
            copy_f(flip(me, o), me).start()

    def greet():
        for load in loads[5:]:
            load.wait()
        pl.semaphore_wait(known, 1)

        @pl.when(border)
        def _():
            pl.semaphore_signal(known, inc=1, device_id=at(me, other), device_id_type=MESH)

    def transform(z):
        return jnp.dot(ahead_v[...], jnp.concatenate([z, z], axis=0), preferred_element_type=F32)

    def analyse(whole, rx, sig, rig=None, step=None):
        whole().wait_recv()
        z = [jnp.concatenate(turn(*[rx[4 * p + n] for n in range(4)], masks_q), axis=0) for p in range(tiles)]
        if step is None:
            for p in range(0, tiles, 2):
                spec = transform(jnp.concatenate(z[p : p + 2], axis=1))
                sig[p] = spec[:, 0:LANES]
                sig[p + 1] = spec[:, LANES:]
            return
        low_w, _ = masks_w
        blank = jnp.zeros(z[0].shape, BF16)
        swapped = [blank] + [pltpu.roll(tile, LANES // 2, 1) for tile in z] + [blank]
        for p in range(tiles):
            shifted = jnp.where(low_w, swapped[p + step], swapped[p + step + 1])
            spec = transform(jnp.concatenate([z[p], shifted], axis=1))
            sig[p] = spec[:, 0:LANES]
            rig[p] = spec[:, LANES:]

    def shift_grads():
        low_f, _ = groups(2 * length, F32)
        for p in range(tiles):
            ahead_of = sigg[p + 1] if p + 1 < tiles else jnp.zeros((2 * length, LANES), F32)
            rigg[p] = pltpu.roll(jnp.where(low_f, ahead_of, sigg[p]), LANES // 2, 1)

    parity = lax.rem(lax.broadcasted_iota(jnp.int32, (8, LANES), 0), 2)
    alt = jnp.where(parity == 0, 1.0, -1.0).astype(F32)
    zero = jnp.zeros((8, LANES), F32)

    def windows(re, im, count=tiles):
        x_re = [zero] + [sigx[p, re, :] for p in range(count)]
        x_im = [zero] + [sigx[p, im, :] for p in range(count)]
        z_re, z_im = [[], []], [[], []]
        for p in range(count):
            before_re, before_im = rigx[p, re, :], rigx[p, im, :]
            z_re[0].append(x_re[p + 1] - alt * before_im)
            z_im[0].append(x_im[p + 1] + alt * before_re)
            z_re[1].append(before_re - alt * x_im[p] if p else before_re)
            z_im[1].append(before_im + alt * x_re[p] if p else before_im)
        return z_re, z_im

    def rows_at(i, start):
        return pl.ds(pl.multiple_of(start + i * 8, 8), 8)

    def correlate(n):
        @pl.loop(0, length // 8, unroll=2)
        def _(i):
            re, im = rows_at(i, 0), rows_at(i, length)
            z_re, z_im = windows(re, im, tiles - 2 * n)
            g_re = {p: sigg[p, re, :] for p in range(2 * n, tiles)}
            g_im = {p: sigg[p, im, :] for p in range(2 * n, tiles)}
            for j in range(4 * n, 4 * n + 4):
                b_re, b_im = z_re[j % 2], z_im[j % 2]
                ms = [(m, m - j // 2) for m in range(j // 2, tiles)]
                acc[j, re, :] = total(g_re[m] * b_re[k] + g_im[m] * b_im[k] for m, k in ms)
                acc[j, im, :] = total(g_im[m] * b_re[k] - g_re[m] * b_im[k] for m, k in ms)

        low_f, even_f = groups(64, F32)
        chunks = [slice(m, m + 64) for m in range(0, 2 * length, 64)]
        for rows in chunks:
            for k in (0, 2):
                a, b = acc[4 * n + k, rows, :], acc[4 * n + k + 1, rows, :]
                moved = pltpu.roll(jnp.where(even_f, b, a), LANES // 4, 1)
                acc[4 * n + k, rows, :] = jnp.where(even_f, a, b) + moved
        for rows in chunks:
            a, b = acc[4 * n, rows, :], acc[4 * n + 2, rows, :]
            moved = pltpu.roll(jnp.where(low_f, b, a), LANES // 2, 1)
            gfs[n, rows, :] = (jnp.where(low_f, a, b) + moved).astype(BF16)

    def inverse(spec):
        return jnp.dot(back_v[...], spec, preferred_element_type=F32).astype(BF16)

    def send_taps(dp, rsem, sets=range(nctx // 4)):
        for n in sets:
            for c in range(4 * n, 4 * n + 4):
                copy_g2(c, dp, rsem).start()

    def send_here(rsem, sets=range(nctx // 4)):
        for n in sets:
            for c in range(4 * n, 4 * n + 4):

                @pl.when(me != c)
                def _():
                    copy_g2(c, row, rsem).start()

    def send_pair(index, sets=range(nctx // 4)):
        @pl.when(part == index)
        def _():
            send_here(g2_rsem, sets)

        @pl.when(part != index)
        def _():
            send_taps(other, g2_rsem, sets)

    def finish_taps(n):
        for m, piece in enumerate(turn_rows(inverse(gfs[n]), masks_q)):
            g2_send[4 * n + m] = piece

    def weigh():
        all_f().wait_recv()
        low_q, even_q = masks_q
        z = []
        for c in range(nctx):
            fa = rxf[c]
            turned = pltpu.roll(fa, LANES // 2, 1)
            pieces = []
            for half in (jnp.where(low_q, fa, turned), jnp.where(low_q, turned, fa)):
                pieces.append(jnp.where(even_q, half, pltpu.roll(half, LANES // 4, 1)))
                pieces.append(jnp.where(even_q, pltpu.roll(half, LANES - LANES // 4, 1), half))
            z.append(jnp.concatenate(pieces, axis=0))
        for p in range(tiles):
            wei[p] = transform(jnp.concatenate(z[2 * p : 2 * p + 2], axis=1))

    def weights(re, im):
        return [[wei[j // 2, rows, pl.ds((j % 2) * LANES, LANES)] for j in range(nctx)] for rows in (re, im)]

    def over_rows(oth, halves):
        @pl.loop(0, length // 16)
        def _(i):
            outs = [halves(rows_at(2 * i + k, 0), rows_at(2 * i + k, length)) for k in range(2)]
            for p in range(tiles):
                for n, start in enumerate((0, length)):
                    rows = pl.ds(pl.multiple_of(start + i * 16, 16), 16)
                    oth[p, rows, :] = jnp.concatenate([outs[0][n][p], outs[1][n][p]], axis=0).astype(BF16)

    def mix_x(re, im):
        w_re, w_im = weights(re, im)
        z_re, z_im = windows(re, im)
        o_re, o_im = [], []
        for p in range(tiles):
            js = [(j, j % 2, p - j // 2) for j in range(2 * p + 2)]
            o_re.append(total(w_re[j] * z_re[h][k] - w_im[j] * z_im[h][k] for j, h, k in js))
            o_im.append(total(w_re[j] * z_im[h][k] + w_im[j] * z_re[h][k] for j, h, k in js))
        return o_re, o_im

    def mix_g(re, im):
        w_re, w_im = weights(re, im)
        g_re = [sigg[p, re, :] for p in range(tiles)]
        g_im = [sigg[p, im, :] for p in range(tiles)]
        z_re, z_im = [[], []], [[], []]
        for p in range(tiles):
            after_re, after_im = rigg[p, re, :], rigg[p, im, :]
            z_re[0].append(g_re[p] + alt * after_im)
            z_im[0].append(g_im[p] - alt * after_re)
            z_re[1].append(after_re + alt * g_im[p + 1] if p + 1 < tiles else after_re)
            z_im[1].append(after_im - alt * g_re[p + 1] if p + 1 < tiles else after_im)
        o_re, o_im = [], []
        for p in range(tiles):
            js = [(j, j % 2, p + j // 2) for j in range(2 * (tiles - p))]
            o_re.append(total(w_re[j] * z_re[h][k] + w_im[j] * z_im[h][k] for j, h, k in js))
            o_im.append(total(w_re[j] * z_im[h][k] - w_im[j] * z_re[h][k] for j, h, k in js))
        return o_re, o_im

    def give_back(oth, send, rx, copy):
        wide = [inverse(jnp.concatenate([oth[p], oth[p + 1]], axis=1)) for p in range(0, tiles, 2)]
        for p in range(tiles):
            for n, piece in enumerate(turn_rows(wide[p // 2][:, p % 2 * LANES : (p % 2 + 1) * LANES], masks_q)):
                send[4 * p + n] = piece
        rx[mine] = send[mine]
        for c in others:
            copy(c, row, mine).start()
            copy(c, other, mine).start()
        copy(me, other, mine).start()

    @pl.when(early)
    def _():
        spread_taps()
        spread_grads()
        greet()
        analyse(all_x, rxx, sigx, rigx, 0)
        weigh()
        over_rows(othx, mix_x)
        give_back(othx, mx_send, mx_rx, copy_mx)
        analyse(all_g, rxg, sigg, rigg, 1)
        correlate(0)
        finish_taps(0)
        send_pair(0, [0])
        over_rows(othg, mix_g)
        give_back(othg, mg_send, mg_rx, copy_mg)
        for n in range(1, nctx // 4):
            correlate(n)
            finish_taps(n)
            send_pair(0, [n])
        for dp in range(ndp // 2, ndp):
            send_taps(dp, g2_rsem)
        send_pair(1)
        g2_rx[slot] = g2_send[me]

    @pl.when(jnp.logical_not(early))
    def _():
        spread_grads()
        spread_taps()
        greet()
        analyse(all_x, rxx, sigx, rigx, 0)
        analyse(all_g, rxg, sigg)
        for n in range(nctx // 4):
            correlate(n)
            finish_taps(n)
            for dp in range(ndp // 2):
                send_taps(dp, g2_rsem, [n])
        send_here(own_rsem)
        weigh()
        shift_grads()
        over_rows(othx, mix_x)
        give_back(othx, mx_send, mx_rx, copy_mx)
        over_rows(othg, mix_g)
        give_back(othg, mg_send, mg_rx, copy_mg)
        g2_rx[slot] = g2_send[me]
        wait_g2(own_rsem, nctx - 1).wait_recv()
        forward(row).start()

    def gate(rx, first, first_out, second, second_out):
        for p in range(tiles):
            cols = slice(p * LANES, (p + 1) * LANES)
            value = jnp.concatenate(turn(*[rx[4 * p + n] for n in range(4)], masks_q), axis=0).astype(F32)
            first_out[0, :, cols] = (first[0, :, cols].astype(F32) * value).astype(BF16)
            second_out[0, :, cols] = (second[0, :, cols].astype(F32) * value).astype(BF16)

    all_mx().wait_recv()
    gate(mx_rx, qv, out_v, gv, gq_v)
    all_mg().wait_recv()
    gate(mg_rx, vv, gk_v, kv, gv_v)

    @pl.when(early)
    def _():
        wait_g2(g2_rsem, ndp * nctx - 1).wait_recv()
        wait_g2(g2_rsem, ndp * nctx - 1).wait_send()

    @pl.when(jnp.logical_not(early))
    def _():
        wait_g2(g2_rsem, ndp // 2 * nctx).wait_recv()
        wait_g2(fwd_rsem, nctx).wait_recv()
        forward(row).wait_send()
        wait_g2(g2_rsem, (ndp // 2 + 1) * nctx - 1).wait_send()

    for whole in (all_x, all_g, all_f, all_mx, all_mg):
        whole().wait_send()


def finish(g2, out, gq, gk, gv, out_hbm, gq_hbm, gk_hbm, gv_hbm, gf_hbm, gf_v, sems):
    length, channels = gf_v.shape
    ql, tiles = length // 4, channels // LANES
    copies = []
    for n, (src, dst) in enumerate(((out, out_hbm), (gq, gq_hbm), (gk, gk_hbm), (gv, gv_hbm), (gf_v, gf_hbm))):
        copies.append(pltpu.make_async_copy(src, dst, sems.at[n]))
    for copy in copies[:4]:
        copy.start()
    masks_f = groups(ql, F32)
    for p in range(tiles):
        cols = slice(p * LANES, (p + 1) * LANES)
        quads = [
            total(g2[2 * tiles * (2 * q + n % 2) + 2 * p + n // 2].astype(F32) for q in range(g2.shape[0] // (4 * tiles)))
            for n in range(4)
        ]
        for n, piece in enumerate(turn(*quads, masks_f)):
            gf_v[n * ql : (n + 1) * ql, cols] = piece
        pltpu.make_async_copy(gf_v.at[:, cols], gf_hbm.at[:, cols], sems.at[4]).start()
    for copy in copies:
        copy.wait()


def fused(nctx, ndp, query, key_input, value_input, filter_taps, grad_output):
    length, channels = query.shape[1], query.shape[2]
    ahead, back = block_tables(length)
    vm = pl.BlockSpec(memory_space=pltpu.VMEM)
    hbm = pl.BlockSpec(memory_space=pltpu.HBM)
    ql, tiles = length // 4, nctx // 2
    dma = pltpu.SemaphoreType.DMA
    kept = 2 * (4 * query.size + ndp * nctx * ql * LANES) + 16384
    pieces = pltpu.VMEM((2 * nctx, ql, LANES), BF16)
    spectrum = pltpu.VMEM((tiles, 2 * length, LANES), F32)
    arrived = pl.pallas_call(
        functools.partial(kernel, nctx, ndp),
        out_shape=(pltpu.VMEM((ndp * nctx, ql, LANES), BF16),) + (pltpu.VMEM(query.shape, BF16),) * 4,
        in_specs=[hbm] * 7,
        out_specs=(vm,) * 5,
        scratch_shapes=[
            pieces,
            pieces,
            pltpu.VMEM(query.shape, BF16),
            pltpu.VMEM(query.shape, BF16),
            pltpu.VMEM(query.shape, BF16),
            pltpu.VMEM(query.shape, BF16),
            pltpu.VMEM((length, channels), F32),
            pltpu.VMEM(ahead.shape, BF16),
            pltpu.VMEM(back.shape, BF16),
            pieces,
            pieces,
            pieces,
            pieces,
            pieces,
            pltpu.VMEM((nctx, ql, LANES), BF16),
            spectrum,
            spectrum,
            spectrum,
            spectrum,
            pltpu.VMEM((tiles, 2 * length, 2 * LANES), F32),
            pltpu.VMEM((tiles, 2 * length, LANES), BF16),
            pltpu.VMEM((tiles, 2 * length, LANES), BF16),
            pltpu.VMEM((nctx, 2 * length, LANES), F32),
            pltpu.VMEM((nctx // 4, 2 * length, LANES), BF16),
            pltpu.VMEM((nctx, ql, LANES), BF16),
            pieces,
            pieces,
            pltpu.SemaphoreType.REGULAR,
            dma((7,)),
        ]
        + [dma] * 15,
        compiler_params=pltpu.CompilerParams(
            collective_id=0, has_side_effects=True, vmem_limit_bytes=VMEM_BYTES - kept
        ),
    )(query, key_input, value_input, filter_taps, grad_output, jnp.asarray(ahead), jnp.asarray(back))
    wide = jax.ShapeDtypeStruct(query.shape, BF16)
    return pl.pallas_call(
        finish,
        out_shape=(wide, wide, wide, wide, jax.ShapeDtypeStruct((length, channels), F32)),
        in_specs=[vm] * 5,
        out_specs=(hbm,) * 5,
        scratch_shapes=[pltpu.VMEM((length, channels), F32), dma((5,))],
        compiler_params=pltpu.CompilerParams(vmem_limit_bytes=16 * 1024 * 1024),
    )(*arrived)


def build_tables(length):
    padded = 2 * length
    columns = 1
    while columns * columns < padded and length % (2 * columns) == 0:
        columns = columns * 2
    row_count = padded // columns
    col_index = jnp.arange(columns, dtype=jnp.int32)
    row_index = jnp.arange(row_count, dtype=jnp.int32)
    col_angle = (col_index[:, None] * col_index[None, :] % columns).astype(jnp.float32) * (
        2.0 * math.pi / columns
    )
    row_angle = (row_index[:, None] * row_index[None, :] % row_count).astype(jnp.float32) * (
        2.0 * math.pi / row_count
    )
    twist_angle = (row_index[:, None] * col_index[None, :] % padded).astype(jnp.float32) * (
        2.0 * math.pi / padded
    )
    return (
        jnp.cos(col_angle),
        -jnp.sin(col_angle),
        jnp.cos(row_angle),
        -jnp.sin(row_angle),
        jnp.cos(twist_angle),
        -jnp.sin(twist_angle),
        row_count,
        columns,
        padded,
    )


def forward(signal, tables):
    col_real, col_imag, row_real, row_imag, twist_real, twist_imag, row_count, columns, padded = (
        tables
    )
    half_rows = row_count // 2
    blocks = signal.reshape(signal.shape[0], half_rows, columns, signal.shape[2])
    section_real = jnp.einsum("kn,snac->scka", row_real[:, :half_rows], blocks, precision=HIGH)
    section_imag = jnp.einsum("kn,snac->scka", row_imag[:, :half_rows], blocks, precision=HIGH)
    turned_real = section_real * twist_real - section_imag * twist_imag
    turned_imag = section_real * twist_imag + section_imag * twist_real
    spec_real = jnp.einsum("scka,aj->sckj", turned_real, col_real, precision=HIGH) - jnp.einsum(
        "scka,aj->sckj", turned_imag, col_imag, precision=HIGH
    )
    spec_imag = jnp.einsum("scka,aj->sckj", turned_real, col_imag, precision=HIGH) + jnp.einsum(
        "scka,aj->sckj", turned_imag, col_real, precision=HIGH
    )
    return (spec_real, spec_imag)


def inverse(spec, tables):
    col_real, col_imag, row_real, row_imag, twist_real, twist_imag, row_count, columns, padded = (
        tables
    )
    spec_real, spec_imag = spec
    half_rows = row_count // 2
    section_real = jnp.einsum("scka,aj->sckj", spec_real, col_real, precision=HIGH) + jnp.einsum(
        "scka,aj->sckj", spec_imag, col_imag, precision=HIGH
    )
    section_imag = jnp.einsum("scka,aj->sckj", spec_imag, col_real, precision=HIGH) - jnp.einsum(
        "scka,aj->sckj", spec_real, col_imag, precision=HIGH
    )
    turned_real = section_real * twist_real + section_imag * twist_imag
    turned_imag = section_imag * twist_real - section_real * twist_imag
    signal = jnp.einsum(
        "nk,scka->snac", row_real[:half_rows], turned_real, precision=HIGH
    ) + jnp.einsum("nk,scka->snac", row_imag[:half_rows], turned_imag, precision=HIGH)
    return signal.reshape(signal.shape[0], half_rows * columns, signal.shape[3]) * (1.0 / padded)


def times_spec(first, second):
    return (
        first[0] * second[0] - first[1] * second[1],
        first[0] * second[1] + first[1] * second[0],
    )


def times_conj(first, second):
    return (
        first[0] * second[0] + first[1] * second[1],
        first[1] * second[0] - first[0] * second[1],
    )


def local(query, key_input, value_input, filter_taps, grad_output):
    product = (key_input.astype(jnp.float32) * value_input.astype(jnp.float32)).astype(jnp.bfloat16)
    grad_mix = (grad_output.astype(jnp.float32) * query.astype(jnp.float32)).astype(jnp.bfloat16)
    owned_filter = lax.all_to_all(filter_taps, "ctx", split_axis=1, concat_axis=0, tiled=True)
    tables = build_tables(owned_filter.shape[0])
    filter_spec = forward(owned_filter[None], tables)
    local_product = lax.all_to_all(product, "ctx", split_axis=2, concat_axis=1, tiled=True)
    prod_spec = forward(local_product.astype(jnp.float32), tables)
    owned_mixed = inverse(times_spec(filter_spec, prod_spec), tables).astype(jnp.bfloat16)
    owned_mixed, prod_spec = (owned_mixed, prod_spec)
    mixed = lax.all_to_all(owned_mixed, "ctx", split_axis=1, concat_axis=2, tiled=True)
    owned_grad = lax.all_to_all(grad_mix, "ctx", split_axis=2, concat_axis=1, tiled=True)
    grad_spec = forward(owned_grad.astype(jnp.float32), tables)
    owned_back = inverse(times_conj(grad_spec, filter_spec), tables).astype(jnp.bfloat16)
    taps_spec = times_conj(grad_spec, prod_spec)
    owned_back, taps_spec = (
        owned_back,
        (jnp.sum(taps_spec[0], axis=0), jnp.sum(taps_spec[1], axis=0)),
    )
    grad_product = lax.all_to_all(owned_back, "ctx", split_axis=1, concat_axis=2, tiled=True)
    mixed_wide = mixed.astype(jnp.float32)
    back_wide = grad_product.astype(jnp.float32)
    output = (query.astype(jnp.float32) * mixed_wide).astype(jnp.bfloat16)
    grad_query = (grad_output.astype(jnp.float32) * mixed_wide).astype(jnp.bfloat16)
    grad_key = (back_wide * value_input.astype(jnp.float32)).astype(jnp.bfloat16)
    grad_value = (back_wide * key_input.astype(jnp.float32)).astype(jnp.bfloat16)
    local_taps = inverse((taps_spec[0][None], taps_spec[1][None]), tables)[0]
    owned_taps = lax.psum(local_taps, "dp")
    grad_filter = lax.all_to_all(owned_taps, "ctx", split_axis=0, concat_axis=1, tiled=True)
    return (output, grad_query, grad_key, grad_value, grad_filter)


def plan(mesh, query, key_input, value_input, filter_taps, grad_output):
    nctx, ndp = mesh.shape["ctx"], mesh.shape["dp"]
    sequences, length, channels = query.shape
    paired = nctx == 2 * ndp and ndp // 2 == 2
    fits = paired and 2 * channels == nctx * LANES and sequences == 1 and length % 64 == 0 and length <= LANES
    run = functools.partial(fused, nctx, ndp) if fits else local
    return run(query, key_input, value_input, filter_taps, grad_output)


def solution(mesh):
    wide, taps = P("dp", "ctx", None), P("ctx", None)
    return jax.shard_map(
        functools.partial(plan, mesh),
        mesh=mesh,
        in_specs=(wide, wide, wide, taps, wide),
        out_specs=(wide, wide, wide, wide, taps),
        check_vma=False,
    )
```

```python
import functools
import math

import jax
import jax.numpy as jnp
import numpy as np
from jax import lax
from jax.experimental import pallas as pl
from jax.experimental.pallas import tpu as pltpu
from jax.sharding import PartitionSpec as P

HIGH = lax.Precision.HIGHEST
MESH = pl.DeviceIdType.MESH
LANES = 128
VMEM_BYTES = 67043328
F32 = jnp.float32
BF16 = jnp.bfloat16


def block_tables(length):
    odd = 2 * np.arange(length, dtype=np.int64)[:, None] + 1
    angle = (odd * np.arange(length, dtype=np.int64)[None, :] % (4 * length)) * (2.0 * math.pi / (4 * length))
    ahead = np.concatenate([np.cos(angle), -np.sin(angle)], axis=0).astype(np.float32)
    back = ahead.T / np.float32(length)

    def split(table):
        high = jnp.asarray(table).astype(BF16)
        low = (jnp.asarray(table) - high.astype(F32)).astype(BF16)
        return high, low

    with jax.ensure_compile_time_eval():
        ahead_high, ahead_low = split(ahead)
        back_high, _ = split(back)
        return (
            np.asarray(jnp.concatenate([ahead_high, ahead_low], axis=1)),
            np.asarray(back_high),
        )


def groups(rows, dtype):
    kind = jnp.int16 if dtype == BF16 else jnp.int32
    lane = lax.broadcasted_iota(kind, (rows, LANES), 1)
    low = lane < LANES // 2
    even = (lane < LANES // 4) | ((lane >= LANES // 2) & (lane < 3 * LANES // 4))
    return low, even


def turn(a, b, c, d, masks):
    low, even = masks

    def halves(first, second):
        turned = pltpu.roll(jnp.where(low, second, first), LANES // 2, 1)
        return jnp.where(low, first, turned), jnp.where(low, turned, second)

    def quarters(first, second):
        return (
            jnp.where(even, first, pltpu.roll(second, LANES // 4, 1)),
            jnp.where(even, pltpu.roll(first, LANES - LANES // 4, 1), second),
        )

    (a, c), (b, d) = halves(a, c), halves(b, d)
    return quarters(a, b) + quarters(c, d)


def turn_rows(tile, masks):
    rows = tile.shape[0] // 4
    return turn(*[tile[n * rows : (n + 1) * rows] for n in range(4)], masks)


def flip(index, mask):
    out, bit = index, 1
    while bit <= mask:
        if mask & bit:
            out = out + bit * (1 - 2 * lax.rem(index // bit, 2))
        bit = 2 * bit
    return out


def total(terms):
    out = None
    for term in terms:
        out = term if out is None else out + term
    return out


def kernel(
    nctx,
    ndp,
    q_hbm,
    k_hbm,
    v_hbm,
    f_hbm,
    g_hbm,
    ahead_hbm,
    back_hbm,
    g2_rx,
    out_v,
    gq_v,
    gk_v,
    gv_v,
    mx_rx,
    mg_rx,
    qv,
    kv,
    vv,
    gv,
    fv,
    ahead_v,
    back_v,
    sendx,
    sendg,
    sendf,
    rxx,
    rxg,
    rxf,
    sigx,
    sigg,
    rigx,
    rigg,
    wei,
    othx,
    othg,
    acc,
    gfs,
    g2_send,
    mx_send,
    mg_send,
    known,
    load_sem,
    x_ssem,
    x_rsem,
    g_ssem,
    g_rsem,
    f_ssem,
    f_rsem,
    g2_ssem,
    g2_rsem,
    own_rsem,
    fwd_ssem,
    fwd_rsem,
    mx_ssem,
    mx_rsem,
    mg_ssem,
    mg_rsem,
):
    me = lax.axis_index("ctx")
    row = lax.axis_index("dp")
    length = qv.shape[1]
    ql = length // 4
    tiles = nctx // 2
    part = lax.rem(row, 2)
    base = row - part
    other = base + 1 - part
    mine = 2 * me + part
    slot = row * nctx + me
    early = row < ndp // 2

    pairs = ((k_hbm, kv), (v_hbm, vv), (g_hbm, gv), (q_hbm, qv), (f_hbm, fv), (ahead_hbm, ahead_v), (back_hbm, back_v))
    loads = [pltpu.make_async_copy(src, dst, load_sem.at[n]) for n, (src, dst) in enumerate(pairs)]
    def at(ctx, dp):
        return {"ctx": ctx, "dp": dp}

    inner = jnp.logical_and(part == 1, row + 1 < ndp)
    outer = jnp.logical_and(part == 0, row > 0)
    across = row + 2 * part - 1
    border = jnp.logical_or(inner, outer)
    barrier = pltpu.get_barrier_semaphore()
    pals = [(other, me)] + [(r, flip(me, o)) for o in range(1, nctx) for r in (row, other)]
    for r, c in reversed(pals):
        pl.semaphore_signal(barrier, inc=1, device_id=at(c, r), device_id_type=MESH)

    @pl.when(border)
    def _():
        pl.semaphore_signal(barrier, inc=1, device_id=at(me, across), device_id_type=MESH)

    for p in range(tiles):
        cols = slice(p * LANES, (p + 1) * LANES)
        for n, (src, dst) in enumerate(pairs[:2]):
            pltpu.make_async_copy(src.at[:, :, cols], dst.at[:, :, cols], load_sem.at[n]).start()
    for load in loads[2:]:
        load.start()
    masks_q, masks_w = groups(ql, BF16), groups(length, BF16)

    def prepare(a_ref, b_ref, into):
        for p in range(tiles):
            cols = slice(p * LANES, (p + 1) * LANES)
            tile = (a_ref[0, :, cols].astype(F32) * b_ref[0, :, cols].astype(F32)).astype(BF16)
            for n, piece in enumerate(turn_rows(tile, masks_q)):
                into[4 * p + n] = piece

    for load in loads[:2]:
        load.wait()
    prepare(kv, vv, sendx)
    rxx[mine] = sendx[mine]
    pl.semaphore_wait(barrier, len(pals) + jnp.where(border, 1, 0))

    def remote(src, dst, ssem, rsem, ctx, dp):
        return pltpu.make_async_remote_copy(
            src_ref=src, dst_ref=dst, send_sem=ssem, recv_sem=rsem, device_id=at(ctx, dp), device_id_type=MESH
        )

    def tile_copy(src, dst, ssem, rsem):
        def copy(ctx, dp, into):
            to = 2 * ctx + lax.rem(dp, 2)
            return remote(src.at[to], dst.at[into], ssem, rsem, ctx, dp)

        def whole():
            every = pl.ds(0, len(pals))
            return remote(src.at[every], dst.at[every], ssem, rsem, me, other)

        return copy, whole

    copy_x, all_x = tile_copy(sendx, rxx, x_ssem, x_rsem)
    copy_g, all_g = tile_copy(sendg, rxg, g_ssem, g_rsem)
    copy_mx, all_mx = tile_copy(mx_send, mx_rx, mx_ssem, mx_rsem)
    copy_mg, all_mg = tile_copy(mg_send, mg_rx, mg_ssem, mg_rsem)

    def copy_f(ctx, into):
        return remote(sendf.at[2 * ctx + part], rxf.at[into], f_ssem, f_rsem, ctx, row)

    def copy_g2(ctx, dp, rsem):
        return remote(g2_send.at[ctx], g2_rx.at[slot], g2_ssem, rsem, ctx, dp)

    def wait_g2(rsem, count):
        every = pl.ds(0, count)
        return remote(g2_rx.at[every], g2_rx.at[every], g2_ssem, rsem, me, other)

    def forward(dp):
        block = pl.ds(pl.multiple_of(dp * nctx, nctx), nctx)
        return remote(g2_rx.at[block], g2_rx.at[block], fwd_ssem, fwd_rsem, me, other)

    def all_f():
        every = pl.ds(0, nctx - 1)
        return remote(sendf.at[every], rxf.at[every], f_ssem, f_rsem, me, other)

    for r, c in pals:
        copy_x(c, r, mine).start()

    @pl.when(border)
    def _():
        pl.semaphore_signal(known, inc=1, device_id=at(me, across), device_id_type=MESH)

    others = [k + jnp.where(me <= k, 1, 0) for k in range(nctx - 1)]

    def spread_grads():
        for load in loads[2:4]:
            load.wait()
        prepare(gv, qv, sendg)
        rxg[mine] = sendg[mine]
        for r, c in pals:
            copy_g(c, r, mine).start()

    def spread_taps():
        loads[4].wait()
        for p in range(tiles):
            for n, piece in enumerate(turn_rows(fv[:, p * LANES : (p + 1) * LANES].astype(BF16), masks_q)):
                sendf[4 * p + n] = piece
        rxf[me] = sendf[mine]
        for o in range(1, nctx):
            copy_f(flip(me, o), me).start()

    def greet():
        for load in loads[5:]:
            load.wait()
        pl.semaphore_wait(known, 1)

        @pl.when(border)
        def _():
            pl.semaphore_signal(known, inc=1, device_id=at(me, other), device_id_type=MESH)

    def transform(z):
        return jnp.dot(ahead_v[...], jnp.concatenate([z, z], axis=0), preferred_element_type=F32)

    def analyse(whole, rx, sig, rig=None, step=None):
        whole().wait_recv()
        z = [jnp.concatenate(turn(*[rx[4 * p + n] for n in range(4)], masks_q), axis=0) for p in range(tiles)]
        if step is None:
            for p in range(0, tiles, 2):
                spec = transform(jnp.concatenate(z[p : p + 2], axis=1))
                sig[p] = spec[:, 0:LANES]
                sig[p + 1] = spec[:, LANES:]
            return
        low_w, _ = masks_w
        blank = jnp.zeros(z[0].shape, BF16)
        swapped = [blank] + [pltpu.roll(tile, LANES // 2, 1) for tile in z] + [blank]
        for p in range(tiles):
            shifted = jnp.where(low_w, swapped[p + step], swapped[p + step + 1])
            spec = transform(jnp.concatenate([z[p], shifted], axis=1))
            sig[p] = spec[:, 0:LANES]
            rig[p] = spec[:, LANES:]

    def shift_grads():
        low_f, _ = groups(2 * length, F32)
        for p in range(tiles):
            ahead_of = sigg[p + 1] if p + 1 < tiles else jnp.zeros((2 * length, LANES), F32)
            rigg[p] = pltpu.roll(jnp.where(low_f, ahead_of, sigg[p]), LANES // 2, 1)

    parity = lax.rem(lax.broadcasted_iota(jnp.int32, (8, LANES), 0), 2)
    alt = jnp.where(parity == 0, 1.0, -1.0).astype(F32)
    zero = jnp.zeros((8, LANES), F32)

    def windows(re, im, count=tiles):
        x_re = [zero] + [sigx[p, re, :] for p in range(count)]
        x_im = [zero] + [sigx[p, im, :] for p in range(count)]
        z_re, z_im = [[], []], [[], []]
        for p in range(count):
            before_re, before_im = rigx[p, re, :], rigx[p, im, :]
            z_re[0].append(x_re[p + 1] - alt * before_im)
            z_im[0].append(x_im[p + 1] + alt * before_re)
            z_re[1].append(before_re - alt * x_im[p] if p else before_re)
            z_im[1].append(before_im + alt * x_re[p] if p else before_im)
        return z_re, z_im

    def rows_at(i, start):
        return pl.ds(pl.multiple_of(start + i * 8, 8), 8)

    def correlate(n):
        @pl.loop(0, length // 8, unroll=2)
        def _(i):
            re, im = rows_at(i, 0), rows_at(i, length)
            z_re, z_im = windows(re, im, tiles - 2 * n)
            g_re = {p: sigg[p, re, :] for p in range(2 * n, tiles)}
            g_im = {p: sigg[p, im, :] for p in range(2 * n, tiles)}
            for j in range(4 * n, 4 * n + 4):
                b_re, b_im = z_re[j % 2], z_im[j % 2]
                ms = [(m, m - j // 2) for m in range(j // 2, tiles)]
                acc[j, re, :] = total(g_re[m] * b_re[k] + g_im[m] * b_im[k] for m, k in ms)
                acc[j, im, :] = total(g_im[m] * b_re[k] - g_re[m] * b_im[k] for m, k in ms)

        low_f, even_f = groups(64, F32)
        chunks = [slice(m, m + 64) for m in range(0, 2 * length, 64)]
        for rows in chunks:
            for k in (0, 2):
                a, b = acc[4 * n + k, rows, :], acc[4 * n + k + 1, rows, :]
                moved = pltpu.roll(jnp.where(even_f, b, a), LANES // 4, 1)
                acc[4 * n + k, rows, :] = jnp.where(even_f, a, b) + moved
        for rows in chunks:
            a, b = acc[4 * n, rows, :], acc[4 * n + 2, rows, :]
            moved = pltpu.roll(jnp.where(low_f, b, a), LANES // 2, 1)
            gfs[n, rows, :] = (jnp.where(low_f, a, b) + moved).astype(BF16)

    def inverse(spec):
        return jnp.dot(back_v[...], spec, preferred_element_type=F32).astype(BF16)

    def send_taps(dp, rsem, sets=range(nctx // 4)):
        for n in sets:
            for c in range(4 * n, 4 * n + 4):
                copy_g2(c, dp, rsem).start()

    def send_here(rsem, sets=range(nctx // 4)):
        for n in sets:
            for c in range(4 * n, 4 * n + 4):

                @pl.when(me != c)
                def _():
                    copy_g2(c, row, rsem).start()

    def send_pair(index, sets=range(nctx // 4)):
        @pl.when(part == index)
        def _():
            send_here(g2_rsem, sets)

        @pl.when(part != index)
        def _():
            send_taps(other, g2_rsem, sets)

    def finish_taps(n):
        for m, piece in enumerate(turn_rows(inverse(gfs[n]), masks_q)):
            g2_send[4 * n + m] = piece

    def weigh():
        all_f().wait_recv()
        low_q, even_q = masks_q
        z = []
        for c in range(nctx):
            fa = rxf[c]
            turned = pltpu.roll(fa, LANES // 2, 1)
            pieces = []
            for half in (jnp.where(low_q, fa, turned), jnp.where(low_q, turned, fa)):
                pieces.append(jnp.where(even_q, half, pltpu.roll(half, LANES // 4, 1)))
                pieces.append(jnp.where(even_q, pltpu.roll(half, LANES - LANES // 4, 1), half))
            z.append(jnp.concatenate(pieces, axis=0))
        for p in range(tiles):
            wei[p] = transform(jnp.concatenate(z[2 * p : 2 * p + 2], axis=1))

    def weights(re, im):
        return [[wei[j // 2, rows, pl.ds((j % 2) * LANES, LANES)] for j in range(nctx)] for rows in (re, im)]

    def over_rows(oth, halves):
        @pl.loop(0, length // 16)
        def _(i):
            outs = [halves(rows_at(2 * i + k, 0), rows_at(2 * i + k, length)) for k in range(2)]
            for p in range(tiles):
                for n, start in enumerate((0, length)):
                    rows = pl.ds(pl.multiple_of(start + i * 16, 16), 16)
                    oth[p, rows, :] = jnp.concatenate([outs[0][n][p], outs[1][n][p]], axis=0).astype(BF16)

    def mix_x(re, im):
        w_re, w_im = weights(re, im)
        z_re, z_im = windows(re, im)
        o_re, o_im = [], []
        for p in range(tiles):
            js = [(j, j % 2, p - j // 2) for j in range(2 * p + 2)]
            o_re.append(total(w_re[j] * z_re[h][k] - w_im[j] * z_im[h][k] for j, h, k in js))
            o_im.append(total(w_re[j] * z_im[h][k] + w_im[j] * z_re[h][k] for j, h, k in js))
        return o_re, o_im

    def mix_g(re, im):
        w_re, w_im = weights(re, im)
        g_re = [sigg[p, re, :] for p in range(tiles)]
        g_im = [sigg[p, im, :] for p in range(tiles)]
        z_re, z_im = [[], []], [[], []]
        for p in range(tiles):
            after_re, after_im = rigg[p, re, :], rigg[p, im, :]
            z_re[0].append(g_re[p] + alt * after_im)
            z_im[0].append(g_im[p] - alt * after_re)
            z_re[1].append(after_re + alt * g_im[p + 1] if p + 1 < tiles else after_re)
            z_im[1].append(after_im - alt * g_re[p + 1] if p + 1 < tiles else after_im)
        o_re, o_im = [], []
        for p in range(tiles):
            js = [(j, j % 2, p + j // 2) for j in range(2 * (tiles - p))]
            o_re.append(total(w_re[j] * z_re[h][k] + w_im[j] * z_im[h][k] for j, h, k in js))
            o_im.append(total(w_re[j] * z_im[h][k] - w_im[j] * z_re[h][k] for j, h, k in js))
        return o_re, o_im

    def give_back(oth, send, rx, copy):
        wide = [inverse(jnp.concatenate([oth[p], oth[p + 1]], axis=1)) for p in range(0, tiles, 2)]
        for p in range(tiles):
            for n, piece in enumerate(turn_rows(wide[p // 2][:, p % 2 * LANES : (p % 2 + 1) * LANES], masks_q)):
                send[4 * p + n] = piece
        rx[mine] = send[mine]
        for c in others:
            copy(c, row, mine).start()
            copy(c, other, mine).start()
        copy(me, other, mine).start()

    @pl.when(early)
    def _():
        spread_taps()
        spread_grads()
        greet()
        analyse(all_x, rxx, sigx, rigx, 0)
        weigh()
        over_rows(othx, mix_x)
        give_back(othx, mx_send, mx_rx, copy_mx)
        analyse(all_g, rxg, sigg, rigg, 1)
        correlate(0)
        finish_taps(0)
        send_pair(0, [0])
        over_rows(othg, mix_g)
        give_back(othg, mg_send, mg_rx, copy_mg)
        for n in range(nctx // 4):
            if n:
                correlate(n)
                finish_taps(n)
            for dp in reversed(range(ndp // 2, ndp)):
                send_taps(dp, g2_rsem, [n])
            if n:
                send_pair(0, [n])
            send_pair(1, [n])
        g2_rx[slot] = g2_send[me]

    @pl.when(jnp.logical_not(early))
    def _():
        spread_grads()
        spread_taps()
        greet()
        analyse(all_x, rxx, sigx, rigx, 0)
        analyse(all_g, rxg, sigg)
        for n in range(nctx // 4):
            correlate(n)
            finish_taps(n)
            for dp in range(ndp // 2):
                send_taps(dp, g2_rsem, [n])
        send_here(own_rsem)
        weigh()
        shift_grads()
        over_rows(othx, mix_x)
        give_back(othx, mx_send, mx_rx, copy_mx)
        over_rows(othg, mix_g)
        give_back(othg, mg_send, mg_rx, copy_mg)
        g2_rx[slot] = g2_send[me]
        wait_g2(own_rsem, nctx - 1).wait_recv()
        forward(row).start()

    def gate(rx, first, first_out, second, second_out):
        for p in range(tiles):
            cols = slice(p * LANES, (p + 1) * LANES)
            value = jnp.concatenate(turn(*[rx[4 * p + n] for n in range(4)], masks_q), axis=0).astype(F32)
            first_out[0, :, cols] = (first[0, :, cols].astype(F32) * value).astype(BF16)
            second_out[0, :, cols] = (second[0, :, cols].astype(F32) * value).astype(BF16)

    all_mx().wait_recv()
    gate(mx_rx, qv, out_v, gv, gq_v)
    all_mg().wait_recv()
    gate(mg_rx, vv, gk_v, kv, gv_v)

    @pl.when(early)
    def _():
        wait_g2(g2_rsem, ndp * nctx - 1).wait_recv()
        wait_g2(g2_rsem, ndp * nctx - 1).wait_send()

    @pl.when(jnp.logical_not(early))
    def _():
        wait_g2(g2_rsem, ndp // 2 * nctx).wait_recv()
        wait_g2(fwd_rsem, nctx).wait_recv()
        forward(row).wait_send()
        wait_g2(g2_rsem, (ndp // 2 + 1) * nctx - 1).wait_send()

    for whole in (all_x, all_g, all_f, all_mx, all_mg):
        whole().wait_send()


def finish(g2, out, gq, gk, gv, out_hbm, gq_hbm, gk_hbm, gv_hbm, gf_hbm, gf_v, sems):
    length, channels = gf_v.shape
    ql, tiles = length // 4, channels // LANES
    copies = []
    for n, (src, dst) in enumerate(((out, out_hbm), (gq, gq_hbm), (gk, gk_hbm), (gv, gv_hbm), (gf_v, gf_hbm))):
        copies.append(pltpu.make_async_copy(src, dst, sems.at[n]))
    for copy in copies[:4]:
        copy.start()
    masks_f = groups(ql, F32)
    for p in range(tiles):
        cols = slice(p * LANES, (p + 1) * LANES)
        quads = [
            total(g2[2 * tiles * (2 * q + n % 2) + 2 * p + n // 2].astype(F32) for q in range(g2.shape[0] // (4 * tiles)))
            for n in range(4)
        ]
        for n, piece in enumerate(turn(*quads, masks_f)):
            gf_v[n * ql : (n + 1) * ql, cols] = piece
        pltpu.make_async_copy(gf_v.at[:, cols], gf_hbm.at[:, cols], sems.at[4]).start()
    for copy in copies:
        copy.wait()


def fused(nctx, ndp, query, key_input, value_input, filter_taps, grad_output):
    length, channels = query.shape[1], query.shape[2]
    ahead, back = block_tables(length)
    vm = pl.BlockSpec(memory_space=pltpu.VMEM)
    hbm = pl.BlockSpec(memory_space=pltpu.HBM)
    ql, tiles = length // 4, nctx // 2
    dma = pltpu.SemaphoreType.DMA
    kept = 2 * (4 * query.size + ndp * nctx * ql * LANES) + 16384
    pieces = pltpu.VMEM((2 * nctx, ql, LANES), BF16)
    spectrum = pltpu.VMEM((tiles, 2 * length, LANES), F32)
    arrived = pl.pallas_call(
        functools.partial(kernel, nctx, ndp),
        out_shape=(pltpu.VMEM((ndp * nctx, ql, LANES), BF16),) + (pltpu.VMEM(query.shape, BF16),) * 4,
        in_specs=[hbm] * 7,
        out_specs=(vm,) * 5,
        scratch_shapes=[
            pieces,
            pieces,
            pltpu.VMEM(query.shape, BF16),
            pltpu.VMEM(query.shape, BF16),
            pltpu.VMEM(query.shape, BF16),
            pltpu.VMEM(query.shape, BF16),
            pltpu.VMEM((length, channels), F32),
            pltpu.VMEM(ahead.shape, BF16),
            pltpu.VMEM(back.shape, BF16),
            pieces,
            pieces,
            pieces,
            pieces,
            pieces,
            pltpu.VMEM((nctx, ql, LANES), BF16),
            spectrum,
            spectrum,
            spectrum,
            spectrum,
            pltpu.VMEM((tiles, 2 * length, 2 * LANES), F32),
            pltpu.VMEM((tiles, 2 * length, LANES), BF16),
            pltpu.VMEM((tiles, 2 * length, LANES), BF16),
            pltpu.VMEM((nctx, 2 * length, LANES), F32),
            pltpu.VMEM((nctx // 4, 2 * length, LANES), BF16),
            pltpu.VMEM((nctx, ql, LANES), BF16),
            pieces,
            pieces,
            pltpu.SemaphoreType.REGULAR,
            dma((7,)),
        ]
        + [dma] * 15,
        compiler_params=pltpu.CompilerParams(
            collective_id=0, has_side_effects=True, vmem_limit_bytes=VMEM_BYTES - kept
        ),
    )(query, key_input, value_input, filter_taps, grad_output, jnp.asarray(ahead), jnp.asarray(back))
    wide = jax.ShapeDtypeStruct(query.shape, BF16)
    return pl.pallas_call(
        finish,
        out_shape=(wide, wide, wide, wide, jax.ShapeDtypeStruct((length, channels), F32)),
        in_specs=[vm] * 5,
        out_specs=(hbm,) * 5,
        scratch_shapes=[pltpu.VMEM((length, channels), F32), dma((5,))],
        compiler_params=pltpu.CompilerParams(vmem_limit_bytes=16 * 1024 * 1024),
    )(*arrived)


def build_tables(length):
    padded = 2 * length
    columns = 1
    while columns * columns < padded and length % (2 * columns) == 0:
        columns = columns * 2
    row_count = padded // columns
    col_index = jnp.arange(columns, dtype=jnp.int32)
    row_index = jnp.arange(row_count, dtype=jnp.int32)
    col_angle = (col_index[:, None] * col_index[None, :] % columns).astype(jnp.float32) * (
        2.0 * math.pi / columns
    )
    row_angle = (row_index[:, None] * row_index[None, :] % row_count).astype(jnp.float32) * (
        2.0 * math.pi / row_count
    )
    twist_angle = (row_index[:, None] * col_index[None, :] % padded).astype(jnp.float32) * (
        2.0 * math.pi / padded
    )
    return (
        jnp.cos(col_angle),
        -jnp.sin(col_angle),
        jnp.cos(row_angle),
        -jnp.sin(row_angle),
        jnp.cos(twist_angle),
        -jnp.sin(twist_angle),
        row_count,
        columns,
        padded,
    )


def forward(signal, tables):
    col_real, col_imag, row_real, row_imag, twist_real, twist_imag, row_count, columns, padded = (
        tables
    )
    half_rows = row_count // 2
    blocks = signal.reshape(signal.shape[0], half_rows, columns, signal.shape[2])
    section_real = jnp.einsum("kn,snac->scka", row_real[:, :half_rows], blocks, precision=HIGH)
    section_imag = jnp.einsum("kn,snac->scka", row_imag[:, :half_rows], blocks, precision=HIGH)
    turned_real = section_real * twist_real - section_imag * twist_imag
    turned_imag = section_real * twist_imag + section_imag * twist_real
    spec_real = jnp.einsum("scka,aj->sckj", turned_real, col_real, precision=HIGH) - jnp.einsum(
        "scka,aj->sckj", turned_imag, col_imag, precision=HIGH
    )
    spec_imag = jnp.einsum("scka,aj->sckj", turned_real, col_imag, precision=HIGH) + jnp.einsum(
        "scka,aj->sckj", turned_imag, col_real, precision=HIGH
    )
    return (spec_real, spec_imag)


def inverse(spec, tables):
    col_real, col_imag, row_real, row_imag, twist_real, twist_imag, row_count, columns, padded = (
        tables
    )
    spec_real, spec_imag = spec
    half_rows = row_count // 2
    section_real = jnp.einsum("scka,aj->sckj", spec_real, col_real, precision=HIGH) + jnp.einsum(
        "scka,aj->sckj", spec_imag, col_imag, precision=HIGH
    )
    section_imag = jnp.einsum("scka,aj->sckj", spec_imag, col_real, precision=HIGH) - jnp.einsum(
        "scka,aj->sckj", spec_real, col_imag, precision=HIGH
    )
    turned_real = section_real * twist_real + section_imag * twist_imag
    turned_imag = section_imag * twist_real - section_real * twist_imag
    signal = jnp.einsum(
        "nk,scka->snac", row_real[:half_rows], turned_real, precision=HIGH
    ) + jnp.einsum("nk,scka->snac", row_imag[:half_rows], turned_imag, precision=HIGH)
    return signal.reshape(signal.shape[0], half_rows * columns, signal.shape[3]) * (1.0 / padded)


def times_spec(first, second):
    return (
        first[0] * second[0] - first[1] * second[1],
        first[0] * second[1] + first[1] * second[0],
    )


def times_conj(first, second):
    return (
        first[0] * second[0] + first[1] * second[1],
        first[1] * second[0] - first[0] * second[1],
    )


def local(query, key_input, value_input, filter_taps, grad_output):
    product = (key_input.astype(jnp.float32) * value_input.astype(jnp.float32)).astype(jnp.bfloat16)
    grad_mix = (grad_output.astype(jnp.float32) * query.astype(jnp.float32)).astype(jnp.bfloat16)
    owned_filter = lax.all_to_all(filter_taps, "ctx", split_axis=1, concat_axis=0, tiled=True)
    tables = build_tables(owned_filter.shape[0])
    filter_spec = forward(owned_filter[None], tables)
    local_product = lax.all_to_all(product, "ctx", split_axis=2, concat_axis=1, tiled=True)
    prod_spec = forward(local_product.astype(jnp.float32), tables)
    owned_mixed = inverse(times_spec(filter_spec, prod_spec), tables).astype(jnp.bfloat16)
    owned_mixed, prod_spec = (owned_mixed, prod_spec)
    mixed = lax.all_to_all(owned_mixed, "ctx", split_axis=1, concat_axis=2, tiled=True)
    owned_grad = lax.all_to_all(grad_mix, "ctx", split_axis=2, concat_axis=1, tiled=True)
    grad_spec = forward(owned_grad.astype(jnp.float32), tables)
    owned_back = inverse(times_conj(grad_spec, filter_spec), tables).astype(jnp.bfloat16)
    taps_spec = times_conj(grad_spec, prod_spec)
    owned_back, taps_spec = (
        owned_back,
        (jnp.sum(taps_spec[0], axis=0), jnp.sum(taps_spec[1], axis=0)),
    )
    grad_product = lax.all_to_all(owned_back, "ctx", split_axis=1, concat_axis=2, tiled=True)
    mixed_wide = mixed.astype(jnp.float32)
    back_wide = grad_product.astype(jnp.float32)
    output = (query.astype(jnp.float32) * mixed_wide).astype(jnp.bfloat16)
    grad_query = (grad_output.astype(jnp.float32) * mixed_wide).astype(jnp.bfloat16)
    grad_key = (back_wide * value_input.astype(jnp.float32)).astype(jnp.bfloat16)
    grad_value = (back_wide * key_input.astype(jnp.float32)).astype(jnp.bfloat16)
    local_taps = inverse((taps_spec[0][None], taps_spec[1][None]), tables)[0]
    owned_taps = lax.psum(local_taps, "dp")
    grad_filter = lax.all_to_all(owned_taps, "ctx", split_axis=0, concat_axis=1, tiled=True)
    return (output, grad_query, grad_key, grad_value, grad_filter)


def plan(mesh, query, key_input, value_input, filter_taps, grad_output):
    nctx, ndp = mesh.shape["ctx"], mesh.shape["dp"]
    sequences, length, channels = query.shape
    paired = nctx == 2 * ndp and ndp // 2 == 2
    fits = paired and 2 * channels == nctx * LANES and sequences == 1 and length % 64 == 0 and length <= LANES
    run = functools.partial(fused, nctx, ndp) if fits else local
    return run(query, key_input, value_input, filter_taps, grad_output)


def solution(mesh):
    wide, taps = P("dp", "ctx", None), P("ctx", None)
    return jax.shard_map(
        functools.partial(plan, mesh),
        mesh=mesh,
        in_specs=(wide, wide, wide, taps, wide),
        out_specs=(wide, wide, wide, wide, taps),
        check_vma=False,
    )
```

```python
import functools
import math

import jax
import jax.numpy as jnp
import numpy as np
from jax import lax
from jax.experimental import pallas as pl
from jax.experimental.pallas import tpu as pltpu
from jax.sharding import PartitionSpec as P

HIGH = lax.Precision.HIGHEST
MESH = pl.DeviceIdType.MESH
LANES = 128
VMEM_BYTES = 67043328
F32 = jnp.float32
BF16 = jnp.bfloat16


def block_tables(length):
    odd = 2 * np.arange(length, dtype=np.int64)[:, None] + 1
    angle = (odd * np.arange(length, dtype=np.int64)[None, :] % (4 * length)) * (2.0 * math.pi / (4 * length))
    ahead = np.concatenate([np.cos(angle), -np.sin(angle)], axis=0).astype(np.float32)
    back = ahead.T / np.float32(length)

    def split(table):
        high = jnp.asarray(table).astype(BF16)
        low = (jnp.asarray(table) - high.astype(F32)).astype(BF16)
        return high, low

    with jax.ensure_compile_time_eval():
        ahead_high, ahead_low = split(ahead)
        back_high, _ = split(back)
        return (
            np.asarray(jnp.concatenate([ahead_high, ahead_low], axis=1)),
            np.asarray(back_high),
        )


def groups(rows, dtype):
    kind = jnp.int16 if dtype == BF16 else jnp.int32
    lane = lax.broadcasted_iota(kind, (rows, LANES), 1)
    low = lane < LANES // 2
    even = (lane < LANES // 4) | ((lane >= LANES // 2) & (lane < 3 * LANES // 4))
    return low, even


def turn(a, b, c, d, masks):
    low, even = masks

    def halves(first, second):
        turned = pltpu.roll(jnp.where(low, second, first), LANES // 2, 1)
        return jnp.where(low, first, turned), jnp.where(low, turned, second)

    def quarters(first, second):
        return (
            jnp.where(even, first, pltpu.roll(second, LANES // 4, 1)),
            jnp.where(even, pltpu.roll(first, LANES - LANES // 4, 1), second),
        )

    (a, c), (b, d) = halves(a, c), halves(b, d)
    return quarters(a, b) + quarters(c, d)


def turn_rows(tile, masks):
    rows = tile.shape[0] // 4
    return turn(*[tile[n * rows : (n + 1) * rows] for n in range(4)], masks)


def flip(index, mask):
    out, bit = index, 1
    while bit <= mask:
        if mask & bit:
            out = out + bit * (1 - 2 * lax.rem(index // bit, 2))
        bit = 2 * bit
    return out


def total(terms):
    out = None
    for term in terms:
        out = term if out is None else out + term
    return out


def kernel(
    nctx,
    ndp,
    q_hbm,
    k_hbm,
    v_hbm,
    f_hbm,
    g_hbm,
    ahead_hbm,
    back_hbm,
    g2_rx,
    out_v,
    gq_v,
    gk_v,
    gv_v,
    mx_rx,
    mg_rx,
    qv,
    kv,
    vv,
    gv,
    fv,
    ahead_v,
    back_v,
    sendx,
    sendg,
    sendf,
    rxx,
    rxg,
    rxf,
    sigx,
    sigg,
    rigx,
    rigg,
    wei,
    othx,
    othg,
    acc,
    gfs,
    g2_send,
    mx_send,
    mg_send,
    known,
    load_sem,
    x_ssem,
    x_rsem,
    g_ssem,
    g_rsem,
    f_ssem,
    f_rsem,
    g2_ssem,
    g2_rsem,
    own_rsem,
    fwd_ssem,
    fwd_rsem,
    mx_ssem,
    mx_rsem,
    mg_ssem,
    mg_rsem,
):
    me = lax.axis_index("ctx")
    row = lax.axis_index("dp")
    length = qv.shape[1]
    ql = length // 4
    tiles = nctx // 2
    part = lax.rem(row, 2)
    base = row - part
    other = base + 1 - part
    mine = 2 * me + part
    slot = row * nctx + me
    early = row < ndp // 2

    pairs = ((k_hbm, kv), (v_hbm, vv), (g_hbm, gv), (q_hbm, qv), (f_hbm, fv), (ahead_hbm, ahead_v), (back_hbm, back_v))
    loads = [pltpu.make_async_copy(src, dst, load_sem.at[n]) for n, (src, dst) in enumerate(pairs)]
    def at(ctx, dp):
        return {"ctx": ctx, "dp": dp}

    inner = jnp.logical_and(part == 1, row + 1 < ndp)
    outer = jnp.logical_and(part == 0, row > 0)
    across = row + 2 * part - 1
    border = jnp.logical_or(inner, outer)
    barrier = pltpu.get_barrier_semaphore()
    pals = [(other, me)] + [(r, flip(me, o)) for o in range(1, nctx) for r in (row, other)]
    for r, c in reversed(pals):
        pl.semaphore_signal(barrier, inc=1, device_id=at(c, r), device_id_type=MESH)

    @pl.when(border)
    def _():
        pl.semaphore_signal(barrier, inc=1, device_id=at(me, across), device_id_type=MESH)

    for p in range(tiles):
        cols = slice(p * LANES, (p + 1) * LANES)
        for n, (src, dst) in enumerate(pairs[:2]):
            pltpu.make_async_copy(src.at[:, :, cols], dst.at[:, :, cols], load_sem.at[n]).start()
    for load in loads[2:]:
        load.start()
    masks_q, masks_w = groups(ql, BF16), groups(length, BF16)

    def prepare(a_ref, b_ref, into):
        for p in range(tiles):
            cols = slice(p * LANES, (p + 1) * LANES)
            tile = (a_ref[0, :, cols].astype(F32) * b_ref[0, :, cols].astype(F32)).astype(BF16)
            for n, piece in enumerate(turn_rows(tile, masks_q)):
                into[4 * p + n] = piece

    for load in loads[:2]:
        load.wait()
    prepare(kv, vv, sendx)
    rxx[mine] = sendx[mine]
    pl.semaphore_wait(barrier, len(pals) + jnp.where(border, 1, 0))

    def remote(src, dst, ssem, rsem, ctx, dp):
        return pltpu.make_async_remote_copy(
            src_ref=src, dst_ref=dst, send_sem=ssem, recv_sem=rsem, device_id=at(ctx, dp), device_id_type=MESH
        )

    def tile_copy(src, dst, ssem, rsem):
        def copy(ctx, dp, into):
            to = 2 * ctx + lax.rem(dp, 2)
            return remote(src.at[to], dst.at[into], ssem, rsem, ctx, dp)

        def whole():
            every = pl.ds(0, len(pals))
            return remote(src.at[every], dst.at[every], ssem, rsem, me, other)

        return copy, whole

    copy_x, all_x = tile_copy(sendx, rxx, x_ssem, x_rsem)
    copy_g, all_g = tile_copy(sendg, rxg, g_ssem, g_rsem)
    copy_mx, all_mx = tile_copy(mx_send, mx_rx, mx_ssem, mx_rsem)
    copy_mg, all_mg = tile_copy(mg_send, mg_rx, mg_ssem, mg_rsem)

    def copy_f(ctx, into):
        return remote(sendf.at[2 * ctx + part], rxf.at[into], f_ssem, f_rsem, ctx, row)

    def copy_g2(ctx, dp, rsem):
        return remote(g2_send.at[ctx], g2_rx.at[slot], g2_ssem, rsem, ctx, dp)

    def wait_g2(rsem, count):
        every = pl.ds(0, count)
        return remote(g2_rx.at[every], g2_rx.at[every], g2_ssem, rsem, me, other)

    def forward(dp):
        block = pl.ds(pl.multiple_of(dp * nctx, nctx), nctx)
        return remote(g2_rx.at[block], g2_rx.at[block], fwd_ssem, fwd_rsem, me, other)

    def all_f():
        every = pl.ds(0, nctx - 1)
        return remote(sendf.at[every], rxf.at[every], f_ssem, f_rsem, me, other)

    for r, c in pals:
        copy_x(c, r, mine).start()

    @pl.when(border)
    def _():
        pl.semaphore_signal(known, inc=1, device_id=at(me, across), device_id_type=MESH)

    others = [k + jnp.where(me <= k, 1, 0) for k in range(nctx - 1)]

    def spread_grads():
        for load in loads[2:4]:
            load.wait()
        prepare(gv, qv, sendg)
        rxg[mine] = sendg[mine]
        for r, c in pals:
            copy_g(c, r, mine).start()

    def spread_taps():
        loads[4].wait()
        for p in range(tiles):
            for n, piece in enumerate(turn_rows(fv[:, p * LANES : (p + 1) * LANES].astype(BF16), masks_q)):
                sendf[4 * p + n] = piece
        rxf[me] = sendf[mine]
        for o in range(1, nctx):
            copy_f(flip(me, o), me).start()

    def greet():
        for load in loads[5:]:
            load.wait()
        pl.semaphore_wait(known, 1)

        @pl.when(border)
        def _():
            pl.semaphore_signal(known, inc=1, device_id=at(me, other), device_id_type=MESH)

    def transform(z):
        return jnp.dot(ahead_v[...], jnp.concatenate([z, z], axis=0), preferred_element_type=F32)

    def analyse(whole, rx, sig, rig=None, step=None):
        whole().wait_recv()
        z = [jnp.concatenate(turn(*[rx[4 * p + n] for n in range(4)], masks_q), axis=0) for p in range(tiles)]
        if step is None:
            for p in range(0, tiles, 2):
                spec = transform(jnp.concatenate(z[p : p + 2], axis=1))
                sig[p] = spec[:, 0:LANES]
                sig[p + 1] = spec[:, LANES:]
            return
        low_w, _ = masks_w
        blank = jnp.zeros(z[0].shape, BF16)
        swapped = [blank] + [pltpu.roll(tile, LANES // 2, 1) for tile in z] + [blank]
        for p in range(tiles):
            shifted = jnp.where(low_w, swapped[p + step], swapped[p + step + 1])
            spec = transform(jnp.concatenate([z[p], shifted], axis=1))
            sig[p] = spec[:, 0:LANES]
            rig[p] = spec[:, LANES:]

    def shift_grads():
        low_f, _ = groups(2 * length, F32)
        for p in range(tiles):
            ahead_of = sigg[p + 1] if p + 1 < tiles else jnp.zeros((2 * length, LANES), F32)
            rigg[p] = pltpu.roll(jnp.where(low_f, ahead_of, sigg[p]), LANES // 2, 1)

    parity = lax.rem(lax.broadcasted_iota(jnp.int32, (8, LANES), 0), 2)
    alt = jnp.where(parity == 0, 1.0, -1.0).astype(F32)
    zero = jnp.zeros((8, LANES), F32)

    def windows(re, im, count=tiles):
        x_re = [zero] + [sigx[p, re, :] for p in range(count)]
        x_im = [zero] + [sigx[p, im, :] for p in range(count)]
        z_re, z_im = [[], []], [[], []]
        for p in range(count):
            before_re, before_im = rigx[p, re, :], rigx[p, im, :]
            z_re[0].append(x_re[p + 1] - alt * before_im)
            z_im[0].append(x_im[p + 1] + alt * before_re)
            z_re[1].append(before_re - alt * x_im[p] if p else before_re)
            z_im[1].append(before_im + alt * x_re[p] if p else before_im)
        return z_re, z_im

    def rows_at(i, start):
        return pl.ds(pl.multiple_of(start + i * 8, 8), 8)

    def correlate(n):
        @pl.loop(0, length // 8, unroll=2)
        def _(i):
            re, im = rows_at(i, 0), rows_at(i, length)
            z_re, z_im = windows(re, im, tiles - 2 * n)
            g_re = {p: sigg[p, re, :] for p in range(2 * n, tiles)}
            g_im = {p: sigg[p, im, :] for p in range(2 * n, tiles)}
            for j in range(4 * n, 4 * n + 4):
                b_re, b_im = z_re[j % 2], z_im[j % 2]
                ms = [(m, m - j // 2) for m in range(j // 2, tiles)]
                acc[j, re, :] = total(g_re[m] * b_re[k] + g_im[m] * b_im[k] for m, k in ms)
                acc[j, im, :] = total(g_im[m] * b_re[k] - g_re[m] * b_im[k] for m, k in ms)

        low_f, even_f = groups(64, F32)
        chunks = [slice(m, m + 64) for m in range(0, 2 * length, 64)]
        for rows in chunks:
            for k in (0, 2):
                a, b = acc[4 * n + k, rows, :], acc[4 * n + k + 1, rows, :]
                moved = pltpu.roll(jnp.where(even_f, b, a), LANES // 4, 1)
                acc[4 * n + k, rows, :] = jnp.where(even_f, a, b) + moved
        for rows in chunks:
            a, b = acc[4 * n, rows, :], acc[4 * n + 2, rows, :]
            moved = pltpu.roll(jnp.where(low_f, b, a), LANES // 2, 1)
            gfs[n, rows, :] = (jnp.where(low_f, a, b) + moved).astype(BF16)

    def inverse(spec):
        return jnp.dot(back_v[...], spec, preferred_element_type=F32).astype(BF16)

    def send_taps(dp, rsem, sets=range(nctx // 4)):
        for n in sets:
            for c in range(4 * n, 4 * n + 4):
                copy_g2(c, dp, rsem).start()

    def send_here(rsem, sets=range(nctx // 4)):
        for n in sets:
            for c in range(4 * n, 4 * n + 4):

                @pl.when(me != c)
                def _():
                    copy_g2(c, row, rsem).start()

    def send_pair(index, sets=range(nctx // 4)):
        @pl.when(part == index)
        def _():
            send_here(g2_rsem, sets)

        @pl.when(part != index)
        def _():
            send_taps(other, g2_rsem, sets)

    def finish_taps(n):
        for m, piece in enumerate(turn_rows(inverse(gfs[n]), masks_q)):
            g2_send[4 * n + m] = piece

    def weigh():
        all_f().wait_recv()
        low_q, even_q = masks_q
        z = []
        for c in range(nctx):
            fa = rxf[c]
            turned = pltpu.roll(fa, LANES // 2, 1)
            pieces = []
            for half in (jnp.where(low_q, fa, turned), jnp.where(low_q, turned, fa)):
                pieces.append(jnp.where(even_q, half, pltpu.roll(half, LANES // 4, 1)))
                pieces.append(jnp.where(even_q, pltpu.roll(half, LANES - LANES // 4, 1), half))
            z.append(jnp.concatenate(pieces, axis=0))
        for p in range(tiles):
            wei[p] = transform(jnp.concatenate(z[2 * p : 2 * p + 2], axis=1))

    def weights(re, im):
        return [[wei[j // 2, rows, pl.ds((j % 2) * LANES, LANES)] for j in range(nctx)] for rows in (re, im)]

    def over_rows(oth, halves):
        @pl.loop(0, length // 16)
        def _(i):
            outs = [halves(rows_at(2 * i + k, 0), rows_at(2 * i + k, length)) for k in range(2)]
            for p in range(tiles):
                for n, start in enumerate((0, length)):
                    rows = pl.ds(pl.multiple_of(start + i * 16, 16), 16)
                    oth[p, rows, :] = jnp.concatenate([outs[0][n][p], outs[1][n][p]], axis=0).astype(BF16)

    def mix_x(re, im):
        w_re, w_im = weights(re, im)
        z_re, z_im = windows(re, im)
        o_re, o_im = [], []
        for p in range(tiles):
            js = [(j, j % 2, p - j // 2) for j in range(2 * p + 2)]
            o_re.append(total(w_re[j] * z_re[h][k] - w_im[j] * z_im[h][k] for j, h, k in js))
            o_im.append(total(w_re[j] * z_im[h][k] + w_im[j] * z_re[h][k] for j, h, k in js))
        return o_re, o_im

    def mix_g(re, im):
        w_re, w_im = weights(re, im)
        g_re = [sigg[p, re, :] for p in range(tiles)]
        g_im = [sigg[p, im, :] for p in range(tiles)]
        z_re, z_im = [[], []], [[], []]
        for p in range(tiles):
            after_re, after_im = rigg[p, re, :], rigg[p, im, :]
            z_re[0].append(g_re[p] + alt * after_im)
            z_im[0].append(g_im[p] - alt * after_re)
            z_re[1].append(after_re + alt * g_im[p + 1] if p + 1 < tiles else after_re)
            z_im[1].append(after_im - alt * g_re[p + 1] if p + 1 < tiles else after_im)
        o_re, o_im = [], []
        for p in range(tiles):
            js = [(j, j % 2, p + j // 2) for j in range(2 * (tiles - p))]
            o_re.append(total(w_re[j] * z_re[h][k] + w_im[j] * z_im[h][k] for j, h, k in js))
            o_im.append(total(w_re[j] * z_im[h][k] - w_im[j] * z_re[h][k] for j, h, k in js))
        return o_re, o_im

    def give_back(oth, send, rx, copy):
        wide = [inverse(jnp.concatenate([oth[p], oth[p + 1]], axis=1)) for p in range(0, tiles, 2)]
        for p in range(tiles):
            for n, piece in enumerate(turn_rows(wide[p // 2][:, p % 2 * LANES : (p % 2 + 1) * LANES], masks_q)):
                send[4 * p + n] = piece
        rx[mine] = send[mine]
        for c in others:
            copy(c, row, mine).start()
            copy(c, other, mine).start()
        copy(me, other, mine).start()

    @pl.when(early)
    def _():
        spread_taps()
        spread_grads()
        greet()
        analyse(all_x, rxx, sigx, rigx, 0)
        weigh()
        over_rows(othx, mix_x)
        give_back(othx, mx_send, mx_rx, copy_mx)
        analyse(all_g, rxg, sigg, rigg, 1)
        correlate(0)
        finish_taps(0)
        send_pair(0, [0])
        over_rows(othg, mix_g)
        give_back(othg, mg_send, mg_rx, copy_mg)
        for n in range(nctx // 4):
            if n:
                correlate(n)
                finish_taps(n)
            for dp in reversed(range(ndp // 2, ndp)):
                send_taps(dp, g2_rsem, [n])
            if n:
                send_pair(0, [n])
            send_pair(1, [n])
        g2_rx[slot] = g2_send[me]

    @pl.when(jnp.logical_not(early))
    def _():
        spread_grads()
        spread_taps()
        greet()
        analyse(all_x, rxx, sigx, rigx, 0)
        analyse(all_g, rxg, sigg)
        for n in range(nctx // 4):
            correlate(n)
            finish_taps(n)
            for dp in range(ndp // 2):
                send_taps(dp, g2_rsem, [n])
        send_here(own_rsem)
        weigh()
        over_rows(othx, mix_x)
        give_back(othx, mx_send, mx_rx, copy_mx)
        shift_grads()
        over_rows(othg, mix_g)
        give_back(othg, mg_send, mg_rx, copy_mg)
        g2_rx[slot] = g2_send[me]
        wait_g2(own_rsem, nctx - 1).wait_recv()
        forward(row).start()

    def gate(rx, first, first_out, second, second_out):
        for p in range(tiles):
            cols = slice(p * LANES, (p + 1) * LANES)
            value = jnp.concatenate(turn(*[rx[4 * p + n] for n in range(4)], masks_q), axis=0).astype(F32)
            first_out[0, :, cols] = (first[0, :, cols].astype(F32) * value).astype(BF16)
            second_out[0, :, cols] = (second[0, :, cols].astype(F32) * value).astype(BF16)

    all_mx().wait_recv()
    gate(mx_rx, qv, out_v, gv, gq_v)
    all_mg().wait_recv()
    gate(mg_rx, vv, gk_v, kv, gv_v)

    @pl.when(early)
    def _():
        wait_g2(g2_rsem, ndp * nctx - 1).wait_recv()
        wait_g2(g2_rsem, ndp * nctx - 1).wait_send()

    @pl.when(jnp.logical_not(early))
    def _():
        wait_g2(g2_rsem, ndp // 2 * nctx).wait_recv()
        wait_g2(fwd_rsem, nctx).wait_recv()
        forward(row).wait_send()
        wait_g2(g2_rsem, (ndp // 2 + 1) * nctx - 1).wait_send()

    for whole in (all_x, all_g, all_f, all_mx, all_mg):
        whole().wait_send()


def finish(g2, out, gq, gk, gv, out_hbm, gq_hbm, gk_hbm, gv_hbm, gf_hbm, gf_v, sems):
    length, channels = gf_v.shape
    ql, tiles = length // 4, channels // LANES
    copies = []
    for n, (src, dst) in enumerate(((out, out_hbm), (gq, gq_hbm), (gk, gk_hbm), (gv, gv_hbm), (gf_v, gf_hbm))):
        copies.append(pltpu.make_async_copy(src, dst, sems.at[n]))
    for copy in copies[:4]:
        copy.start()
    masks_f = groups(ql, F32)
    for p in range(tiles):
        cols = slice(p * LANES, (p + 1) * LANES)
        quads = [
            total(g2[2 * tiles * (2 * q + n % 2) + 2 * p + n // 2].astype(F32) for q in range(g2.shape[0] // (4 * tiles)))
            for n in range(4)
        ]
        for n, piece in enumerate(turn(*quads, masks_f)):
            gf_v[n * ql : (n + 1) * ql, cols] = piece
        pltpu.make_async_copy(gf_v.at[:, cols], gf_hbm.at[:, cols], sems.at[4]).start()
    for copy in copies:
        copy.wait()


def fused(nctx, ndp, query, key_input, value_input, filter_taps, grad_output):
    length, channels = query.shape[1], query.shape[2]
    ahead, back = block_tables(length)
    vm = pl.BlockSpec(memory_space=pltpu.VMEM)
    hbm = pl.BlockSpec(memory_space=pltpu.HBM)
    ql, tiles = length // 4, nctx // 2
    dma = pltpu.SemaphoreType.DMA
    kept = 2 * (4 * query.size + ndp * nctx * ql * LANES) + 16384
    pieces = pltpu.VMEM((2 * nctx, ql, LANES), BF16)
    spectrum = pltpu.VMEM((tiles, 2 * length, LANES), F32)
    arrived = pl.pallas_call(
        functools.partial(kernel, nctx, ndp),
        out_shape=(pltpu.VMEM((ndp * nctx, ql, LANES), BF16),) + (pltpu.VMEM(query.shape, BF16),) * 4,
        in_specs=[hbm] * 7,
        out_specs=(vm,) * 5,
        scratch_shapes=[
            pieces,
            pieces,
            pltpu.VMEM(query.shape, BF16),
            pltpu.VMEM(query.shape, BF16),
            pltpu.VMEM(query.shape, BF16),
            pltpu.VMEM(query.shape, BF16),
            pltpu.VMEM((length, channels), F32),
            pltpu.VMEM(ahead.shape, BF16),
            pltpu.VMEM(back.shape, BF16),
            pieces,
            pieces,
            pieces,
            pieces,
            pieces,
            pltpu.VMEM((nctx, ql, LANES), BF16),
            spectrum,
            spectrum,
            spectrum,
            spectrum,
            pltpu.VMEM((tiles, 2 * length, 2 * LANES), F32),
            pltpu.VMEM((tiles, 2 * length, LANES), BF16),
            pltpu.VMEM((tiles, 2 * length, LANES), BF16),
            pltpu.VMEM((nctx, 2 * length, LANES), F32),
            pltpu.VMEM((nctx // 4, 2 * length, LANES), BF16),
            pltpu.VMEM((nctx, ql, LANES), BF16),
            pieces,
            pieces,
            pltpu.SemaphoreType.REGULAR,
            dma((7,)),
        ]
        + [dma] * 15,
        compiler_params=pltpu.CompilerParams(
            collective_id=0, has_side_effects=True, vmem_limit_bytes=VMEM_BYTES - kept
        ),
    )(query, key_input, value_input, filter_taps, grad_output, jnp.asarray(ahead), jnp.asarray(back))
    wide = jax.ShapeDtypeStruct(query.shape, BF16)
    return pl.pallas_call(
        finish,
        out_shape=(wide, wide, wide, wide, jax.ShapeDtypeStruct((length, channels), F32)),
        in_specs=[vm] * 5,
        out_specs=(hbm,) * 5,
        scratch_shapes=[pltpu.VMEM((length, channels), F32), dma((5,))],
        compiler_params=pltpu.CompilerParams(vmem_limit_bytes=16 * 1024 * 1024),
    )(*arrived)


def build_tables(length):
    padded = 2 * length
    columns = 1
    while columns * columns < padded and length % (2 * columns) == 0:
        columns = columns * 2
    row_count = padded // columns
    col_index = jnp.arange(columns, dtype=jnp.int32)
    row_index = jnp.arange(row_count, dtype=jnp.int32)
    col_angle = (col_index[:, None] * col_index[None, :] % columns).astype(jnp.float32) * (
        2.0 * math.pi / columns
    )
    row_angle = (row_index[:, None] * row_index[None, :] % row_count).astype(jnp.float32) * (
        2.0 * math.pi / row_count
    )
    twist_angle = (row_index[:, None] * col_index[None, :] % padded).astype(jnp.float32) * (
        2.0 * math.pi / padded
    )
    return (
        jnp.cos(col_angle),
        -jnp.sin(col_angle),
        jnp.cos(row_angle),
        -jnp.sin(row_angle),
        jnp.cos(twist_angle),
        -jnp.sin(twist_angle),
        row_count,
        columns,
        padded,
    )


def forward(signal, tables):
    col_real, col_imag, row_real, row_imag, twist_real, twist_imag, row_count, columns, padded = (
        tables
    )
    half_rows = row_count // 2
    blocks = signal.reshape(signal.shape[0], half_rows, columns, signal.shape[2])
    section_real = jnp.einsum("kn,snac->scka", row_real[:, :half_rows], blocks, precision=HIGH)
    section_imag = jnp.einsum("kn,snac->scka", row_imag[:, :half_rows], blocks, precision=HIGH)
    turned_real = section_real * twist_real - section_imag * twist_imag
    turned_imag = section_real * twist_imag + section_imag * twist_real
    spec_real = jnp.einsum("scka,aj->sckj", turned_real, col_real, precision=HIGH) - jnp.einsum(
        "scka,aj->sckj", turned_imag, col_imag, precision=HIGH
    )
    spec_imag = jnp.einsum("scka,aj->sckj", turned_real, col_imag, precision=HIGH) + jnp.einsum(
        "scka,aj->sckj", turned_imag, col_real, precision=HIGH
    )
    return (spec_real, spec_imag)


def inverse(spec, tables):
    col_real, col_imag, row_real, row_imag, twist_real, twist_imag, row_count, columns, padded = (
        tables
    )
    spec_real, spec_imag = spec
    half_rows = row_count // 2
    section_real = jnp.einsum("scka,aj->sckj", spec_real, col_real, precision=HIGH) + jnp.einsum(
        "scka,aj->sckj", spec_imag, col_imag, precision=HIGH
    )
    section_imag = jnp.einsum("scka,aj->sckj", spec_imag, col_real, precision=HIGH) - jnp.einsum(
        "scka,aj->sckj", spec_real, col_imag, precision=HIGH
    )
    turned_real = section_real * twist_real + section_imag * twist_imag
    turned_imag = section_imag * twist_real - section_real * twist_imag
    signal = jnp.einsum(
        "nk,scka->snac", row_real[:half_rows], turned_real, precision=HIGH
    ) + jnp.einsum("nk,scka->snac", row_imag[:half_rows], turned_imag, precision=HIGH)
    return signal.reshape(signal.shape[0], half_rows * columns, signal.shape[3]) * (1.0 / padded)


def times_spec(first, second):
    return (
        first[0] * second[0] - first[1] * second[1],
        first[0] * second[1] + first[1] * second[0],
    )


def times_conj(first, second):
    return (
        first[0] * second[0] + first[1] * second[1],
        first[1] * second[0] - first[0] * second[1],
    )


def local(query, key_input, value_input, filter_taps, grad_output):
    product = (key_input.astype(jnp.float32) * value_input.astype(jnp.float32)).astype(jnp.bfloat16)
    grad_mix = (grad_output.astype(jnp.float32) * query.astype(jnp.float32)).astype(jnp.bfloat16)
    owned_filter = lax.all_to_all(filter_taps, "ctx", split_axis=1, concat_axis=0, tiled=True)
    tables = build_tables(owned_filter.shape[0])
    filter_spec = forward(owned_filter[None], tables)
    local_product = lax.all_to_all(product, "ctx", split_axis=2, concat_axis=1, tiled=True)
    prod_spec = forward(local_product.astype(jnp.float32), tables)
    owned_mixed = inverse(times_spec(filter_spec, prod_spec), tables).astype(jnp.bfloat16)
    owned_mixed, prod_spec = (owned_mixed, prod_spec)
    mixed = lax.all_to_all(owned_mixed, "ctx", split_axis=1, concat_axis=2, tiled=True)
    owned_grad = lax.all_to_all(grad_mix, "ctx", split_axis=2, concat_axis=1, tiled=True)
    grad_spec = forward(owned_grad.astype(jnp.float32), tables)
    owned_back = inverse(times_conj(grad_spec, filter_spec), tables).astype(jnp.bfloat16)
    taps_spec = times_conj(grad_spec, prod_spec)
    owned_back, taps_spec = (
        owned_back,
        (jnp.sum(taps_spec[0], axis=0), jnp.sum(taps_spec[1], axis=0)),
    )
    grad_product = lax.all_to_all(owned_back, "ctx", split_axis=1, concat_axis=2, tiled=True)
    mixed_wide = mixed.astype(jnp.float32)
    back_wide = grad_product.astype(jnp.float32)
    output = (query.astype(jnp.float32) * mixed_wide).astype(jnp.bfloat16)
    grad_query = (grad_output.astype(jnp.float32) * mixed_wide).astype(jnp.bfloat16)
    grad_key = (back_wide * value_input.astype(jnp.float32)).astype(jnp.bfloat16)
    grad_value = (back_wide * key_input.astype(jnp.float32)).astype(jnp.bfloat16)
    local_taps = inverse((taps_spec[0][None], taps_spec[1][None]), tables)[0]
    owned_taps = lax.psum(local_taps, "dp")
    grad_filter = lax.all_to_all(owned_taps, "ctx", split_axis=0, concat_axis=1, tiled=True)
    return (output, grad_query, grad_key, grad_value, grad_filter)


def plan(mesh, query, key_input, value_input, filter_taps, grad_output):
    nctx, ndp = mesh.shape["ctx"], mesh.shape["dp"]
    sequences, length, channels = query.shape
    paired = nctx == 2 * ndp and ndp // 2 == 2
    fits = paired and 2 * channels == nctx * LANES and sequences == 1 and length % 64 == 0 and length <= LANES
    run = functools.partial(fused, nctx, ndp) if fits else local
    return run(query, key_input, value_input, filter_taps, grad_output)


def solution(mesh):
    wide, taps = P("dp", "ctx", None), P("ctx", None)
    return jax.shard_map(
        functools.partial(plan, mesh),
        mesh=mesh,
        in_specs=(wide, wide, wide, taps, wide),
        out_specs=(wide, wide, wide, wide, taps),
        check_vma=False,
    )
```
